32 devices in a mesh: ctx: 8 (over y, x, core), tp: 4 (over z).
Axes of the slice: x: 2, y: 2, z: 4, core: 2. Of those that a mesh axis runs over, the one named last changes fastest.
Arguments:
- hidden: bfloat16 [2048, 8192], P('ctx', 'tp'), may hold values from -6 to 6
- queries: bfloat16 [2048, 4096], P('ctx', 'tp'), may hold values from -1000 to 1000
- kv_weight: bfloat16 [8192, 1024], P('tp', 'ctx'), may hold values from -0.0625 to 0.0625
- kv_bias: bfloat16 [1024], P('tp'), may hold values from -3 to 3
- window: int32 [4], P('tp'), may hold values from 1024 to 4096, as said below
- segment_ids: int32 [2048], P('ctx'), may hold values from 0 to 3, never falling along the last dimension, each value on 1 to 1024 neighbouring positions
Outputs:
- attended: bfloat16 [2048, 4096], P('ctx', 'tp')
- kv_cache: bfloat16 [2048, 1024], P('ctx', 'tp')
The draws below stay inside these ranges and needn't reach their ends.
Inputs may be any that keep to these rules, and one draw needn't show every extreme that they name: `window`: each entry is 1024 to 4096; some key head's entry equals 4096.
All inputs are finite; a program needn't handle non-finite values.
Results may differ from the reference program's by a relative error of at most 0.012.
Values may be sent and summed in bfloat16 or wider, within the bound.
A program may use at most 64 MiB of HBM per device.

```python
import math
import jax
import jax.numpy as jnp
import numpy as np
from jax import lax

D = 8192
HD = 128
KVH = 4
QPK = 8
WINDOW = 4096
TOK_DEV = 256
TOKENS = 2048
HALO = 16
N_CTX = 8


def draw_window(key, part):
    first_key, second_key = jax.random.split(jax.random.fold_in(key, 11))
    widths = jax.random.randint(first_key, (KVH,), WINDOW // 4, WINDOW + 1)
    longest = jax.random.randint(second_key, (), 0, KVH)
    return jnp.where(jnp.arange(KVH) == longest, WINDOW, widths).astype(jnp.int32)


def draw_queries(key, part):
    subkeys = jax.random.split(jax.random.fold_in(key, 12), 1)
    normals = jnp.clip(jax.random.normal(subkeys[0], (TOKENS, KVH * QPK * HD), jnp.float32), -6.0, 6.0)
    return normals.astype(jnp.bfloat16)


def levels(stream_key, extent, pieces, smallest, largest):
    gain, own = 1.0, jax.random.fold_in(stream_key, 6)
    for axis_at, parts in pieces:
        draws = jnp.exp(jax.random.uniform(jax.random.fold_in(own, axis_at), (parts,), jnp.float32, smallest / len(pieces), largest / len(pieces)))
        gain = gain * jnp.repeat(draws, extent[axis_at] // parts).reshape([-1 if axis == axis_at else 1 for axis in range(len(extent))])
    return gain


def profile(amount, total, most, lean):
    portions = [(1 << 20) // math.isqrt(grade ** lean) + 1 for grade in range(2, amount + 1)]
    rest, given = total - most - (amount - 1), [1] * (amount - 1)
    while rest > 0:
        movable = [i for i in range(amount - 1) if given[i] < most]
        pool, budget = sum([portions[i] for i in movable]), rest
        for i in movable:
            addition = min(most - given[i], max(1, budget * portions[i] // pool), rest)
            given[i] = given[i] + addition
            rest = rest - addition
    return np.array([most] + given)


def uneven_parts(rng, amount, total, bound, skew):
    if amount == 2:
        one = jax.random.randint(rng, (), max(1, total - bound), min(bound, total - 1) + 1)
        return jnp.stack([one, total - one])
    lengths = jnp.asarray(profile(amount, total, bound, skew), jnp.int32)
    couples = (amount - 1) // 2
    giver, taker = lengths[1:1 + 2 * couples:2], lengths[2:2 + 2 * couples:2]
    slack = jnp.minimum(giver - 1, bound - taker)
    passed = jax.random.randint(jax.random.fold_in(rng, 1), (couples,), 0, 1 << 20) % (slack + 1)
    lengths = lengths.at[1:1 + 2 * couples:2].set(giver - passed).at[2:2 + 2 * couples:2].set(taker + passed)
    return lengths[jax.random.permutation(jax.random.fold_in(rng, 2), amount)]


def gaussian(key, extent, spread, most, shards=(), held_as=jnp.bfloat16):
    values = spread * jax.random.normal(key, extent, jnp.float32)
    if shards:
        values = values * levels(key, extent, shards, -0.22, 0.18)
    return jnp.clip(values, -most, most).astype(held_as)


def setup_inputs(seed: int = 0) -> dict:
    key_of = jax.random.split(jax.random.key(seed), 7)
    return {
        "hidden": gaussian(key_of[0], (TOKENS, D), 1.0, 6.0, ((0, 8), (1, 4))),
        "queries": draw_queries(jax.random.fold_in(key_of[6], 71), 0),
        "kv_weight": gaussian(key_of[2], (D, KVH * 2 * HD), D ** -0.5, 0.0625, ((0, 4), (1, 8))),
        "kv_bias": gaussian(key_of[3], (KVH * 2 * HD,), 0.5, 3.0, ((0, 4),)),
        "window": draw_window(jax.random.fold_in(key_of[6], 71), 0),
        "segment_ids": jnp.searchsorted(jnp.cumsum(uneven_parts(key_of[5], max(4, TOKENS // (WINDOW // 2)), TOKENS, min(WINDOW, TOKENS // 2), 1)), jnp.arange(TOKENS), side="right").astype(jnp.int32),
    }


rope_base = 1000000.0


def rotate(values, positions):
    half = values.shape[-1] // 2
    freqs = rope_base ** (-2.0 * jnp.arange(half, dtype=jnp.float32) / values.shape[-1])
    angles = positions.astype(jnp.float32)[:, None, None] * freqs[None, None, :]
    cosine = jnp.cos(angles)
    sine = jnp.sin(angles)
    former = values[..., :half]
    latter = values[..., half:]
    return jnp.concatenate([former * cosine - latter * sine, latter * cosine + former * sine], axis=-1)


def reference(hidden, queries, kv_weight, kv_bias, window, segment_ids):
    projected = jnp.dot(hidden, kv_weight, preferred_element_type=jnp.float32) + kv_bias.astype(jnp.float32)[None, :]
    projected = projected.reshape(TOKENS, KVH, 2, HD)
    positions = jnp.arange(TOKENS, dtype=jnp.int32)
    rotated = rotate(projected[:, :, 0], positions)
    cache = jnp.stack([rotated, projected[:, :, 1]], axis=2).astype(jnp.bfloat16)
    cache = lax.optimization_barrier(cache)
    padding = HALO * TOK_DEV
    padded = jnp.concatenate([jnp.zeros((padding, KVH, 2, HD), jnp.bfloat16), cache], axis=0)
    padded_seg = jnp.concatenate([jnp.full((padding,), -1, jnp.int32), segment_ids], axis=0)
    query_all = queries.reshape(TOKENS, KVH, QPK, HD)

    def one_block(block):
        start = (block * TOK_DEV).astype(jnp.int32)
        keys_here = lax.dynamic_slice_in_dim(padded, start, padding + TOK_DEV, 0).astype(jnp.float32)
        seg_here = lax.dynamic_slice_in_dim(padded_seg, start, padding + TOK_DEV, 0)
        key_pos = start - padding + jnp.arange(padding + TOK_DEV, dtype=jnp.int32)
        query_here = lax.dynamic_slice_in_dim(query_all, start, TOK_DEV, 0).astype(jnp.float32)
        query_pos = start + jnp.arange(TOK_DEV, dtype=jnp.int32)
        query_seg = lax.dynamic_slice_in_dim(segment_ids, start, TOK_DEV, 0)
        scores = jnp.einsum("tkgd,skd->ktgs", query_here, keys_here[:, :, 0]) * HD ** -0.5
        gap = query_pos[:, None] - key_pos[None, :]
        allowed = (query_seg[:, None] == seg_here[None, :]) & (gap >= 0) & (key_pos >= 0)[None, :]
        allowed = allowed[None, :, None, :] & (gap[None, :, None, :] < window[:, None, None, None])
        scores = jnp.where(allowed, scores, -jnp.inf)
        highest = jnp.max(scores, axis=-1, keepdims=True)
        probs = jnp.exp(scores - highest)
        totals = jnp.sum(probs, axis=-1)
        rounded = lax.optimization_barrier(probs.astype(jnp.bfloat16)).astype(jnp.float32)
        mixed = jnp.einsum("ktgs,skd->tkgd", rounded, keys_here[:, :, 1])
        mixed = mixed / jnp.transpose(totals, (1, 0, 2))[..., None]
        return mixed.astype(jnp.bfloat16).reshape(TOK_DEV, KVH * QPK * HD)

    attended = lax.map(one_block, jnp.arange(N_CTX, dtype=jnp.int32)).reshape(TOKENS, KVH * QPK * HD)
    return attended, cache.reshape(TOKENS, KVH * 2 * HD)
```

```python
import functools

import jax
import jax.numpy as jnp
import numpy as np
from jax import lax
from jax.experimental import pallas as pl
from jax.experimental.pallas import tpu as pltpu
from jax.sharding import PartitionSpec as P

WINDOW = 4096
MESH = pl.DeviceIdType.MESH
LOG2E = 1.4426950408889634


rope_base = 1000000.0


def passed_along(value, axis, steps):
    count = lax.axis_size(axis)
    initial, last = (max(0, -steps), min(count, count - steps))
    return lax.ppermute(value, axis, [(source, source + steps) for source in range(initial, last)])


def rotate(values, positions):
    half = values.shape[-1] // 2
    freqs = rope_base ** (-2.0 * jnp.arange(half, dtype=jnp.float32) / values.shape[-1])
    angles = positions.astype(jnp.float32)[:, None] * freqs[None, :]
    cosine = jnp.cos(angles)
    sine = jnp.sin(angles)
    former = values[:, :half]
    latter = values[:, half:]
    return jnp.concatenate(
        [former * cosine - latter * sine, latter * cosine + former * sine], axis=1
    )


def attend(carry, query_rows, query_pos, query_seg, reach, block, block_seg, block_pos):
    running_max, running_sum, weighted = carry
    head = block.shape[1] // 2
    scores = lax.dot_general(
        query_rows, block[:, :head], (((1,), (1,)), ((), ())), preferred_element_type=jnp.float32
    )
    scores = scores * head ** (-0.5)
    gap = query_pos[:, None] - block_pos[None, :]
    allowed = (
        (query_seg[:, None] == block_seg[None, :])
        & (gap >= 0)
        & (gap < reach)
        & (block_pos >= 0)[None, :]
    )
    scores = jnp.where(allowed, scores, -jnp.inf)
    newest = jnp.maximum(running_max, jnp.max(scores, axis=1))
    probs = jnp.exp(scores - newest[:, None])
    rescale = jnp.exp(running_max - newest)
    summed = running_sum * rescale + jnp.sum(probs, axis=1)
    mixed = jnp.dot(probs.astype(jnp.bfloat16), block[:, head:], preferred_element_type=jnp.float32)
    return (newest, summed, weighted * rescale[:, None] + mixed)


def body(hidden, queries, kv_weight, kv_bias, window, segment_ids):
    tok_rows = hidden.shape[0]
    terms = jnp.dot(
        hidden,
        lax.all_gather(kv_weight, "ctx", axis=1, tiled=True),
        preferred_element_type=jnp.float32,
    )
    projected = lax.psum_scatter(terms, "tp", scatter_dimension=1, tiled=True)
    projected = projected + kv_bias.astype(jnp.float32)[None, :]
    head = kv_bias.shape[0] // 2
    shard = lax.axis_index("ctx")
    offsets = jnp.arange(tok_rows, dtype=jnp.int32)
    positions = shard * tok_rows + offsets
    cache = jnp.concatenate(
        [rotate(projected[:, :head], positions), projected[:, head:]], axis=1
    ).astype(jnp.bfloat16)
    group = queries.shape[1] // head
    query_rows = queries.reshape(tok_rows * group, head)
    query_pos = jnp.repeat(positions, group)
    query_seg = jnp.repeat(segment_ids, group)
    reach = window[0]

    def absorb(carry, block, block_seg, block_pos):
        return attend(carry, query_rows, query_pos, query_seg, reach, block, block_seg, block_pos)

    row_count = tok_rows * group
    carry = (
        jnp.full((row_count,), -jnp.inf, jnp.float32),
        jnp.zeros((row_count,), jnp.float32),
        jnp.zeros((row_count, head), jnp.float32),
    )
    carry = absorb(carry, cache, segment_ids, positions)
    halo_count = WINDOW // tok_rows
    held_kv = cache
    held_seg = segment_ids
    have = 0
    while have < halo_count:
        got_kv, got_seg = passed_along((held_kv, held_seg), "ctx", max(have, 1))
        shards = got_kv.shape[0] // tok_rows
        for member in range(shards):
            lower = member * tok_rows
            block_pos = (shard - have - shards + member) * tok_rows + offsets
            carry = absorb(
                carry,
                got_kv[lower : lower + tok_rows],
                got_seg[lower : lower + tok_rows],
                block_pos,
            )
        if have == 0:
            held_kv, held_seg = (got_kv, got_seg)
        else:
            held_kv = jnp.concatenate([got_kv, held_kv], axis=0)
            held_seg = jnp.concatenate([got_seg, held_seg], axis=0)
        have = have + shards
    newest, summed, weighted = carry
    attended = (weighted / summed[:, None]).reshape(tok_rows, group * head).astype(jnp.bfloat16)
    return (attended, cache)


def fused_kernel(
    halo, back, window_ref, hid_hbm, w_hbm, q_hbm, bias_hbm, freq_hbm, seg_hbm, out_ref, cache_ref,
    kv_ref, segs_ref, hbuf, wbuf, part_out, part_in, own, cosb, sinb,
    q_ref, bias_ref, freq_ref, seg_line, seg_ref, mask, probs, totals,
    local_sem, hid_sem, gate, wsend, wrecv, psend, precv, ksend, krecv, fsend, frecv, ssend, srecv,
):
    c = lax.axis_index("ctx")
    t = lax.axis_index("tp")
    n_ctx = lax.axis_size("ctx")
    n_tp = lax.axis_size("tp")
    pairs = n_ctx // 2
    pair = c // 2
    core = c % 2
    mate = pair * 2 + (1 - core)
    toks = hid_hbm.shape[0]
    feats, head = w_hbm.shape
    half = feats // 2
    span = 2 * toks
    own_rows = pl.ds(pl.multiple_of(core * toks, toks), toks)

    load_w = [
        pltpu.make_async_copy(w_hbm.at[pl.ds(q * half, half)], wbuf.at[0, q], local_sem.at[q])
        for q in range(2)
    ]
    load_h = pltpu.make_async_copy(hid_hbm, hbuf.at[own_rows], local_sem.at[2])
    small = [
        pltpu.make_async_copy(src, dst, local_sem.at[3 + at])
        for at, (src, dst) in enumerate(
            [(seg_hbm, seg_line), (bias_hbm, bias_ref), (freq_hbm, freq_ref), (q_hbm, q_ref)]
        )
    ]
    load_w[0].start()
    load_w[1].start()
    load_h.start()
    for copy in small:
        copy.start()

    barrier = pltpu.get_barrier_semaphore()
    for step in range(1, n_ctx):
        pl.semaphore_signal(barrier, inc=1, device_id=((c + step) % n_ctx, t), device_id_type=MESH)
    for step in range(1, n_tp):
        pl.semaphore_signal(barrier, inc=1, device_id=(c, (t + step) % n_tp), device_id_type=MESH)
    pl.semaphore_wait(barrier, n_ctx + n_tp - 2)

    def neighbour(d):
        other_x = 1 - pair % 2 if d % 2 else pair % 2
        other_y = 1 - pair // 2 if d // 2 else pair // 2
        return other_y * 2 + other_x

    def w_copy(src, dst, q, sem, to):
        return pltpu.make_async_remote_copy(
            src_ref=wbuf.at[src, q], dst_ref=wbuf.at[dst, q],
            send_sem=wsend.at[sem], recv_sem=wrecv.at[dst, q],
            device_id=(2 * neighbour(to) + core, t), device_id_type=MESH,
        )

    x_first, x_second = w_copy(0, 1, 0, 0, 1), w_copy(0, 1, 1, 1, 1)
    y_first, y_second = w_copy(0, 2, 1, 2, 2), w_copy(0, 2, 0, 3, 2)
    relay_y, relay_x = w_copy(1, 3, 0, 4, 2), w_copy(2, 3, 1, 5, 1)

    def send_weights():
        x_first.start()
        y_first.start()
        x_second.start()
        y_second.start()

    load_w[0].wait()
    load_w[1].wait()

    @pl.when(core == 0)
    def _():
        send_weights()

    load_h.wait()
    hid = pltpu.make_async_remote_copy(
        src_ref=hbuf.at[own_rows], dst_ref=hbuf.at[own_rows],
        send_sem=hid_sem.at[0], recv_sem=hid_sem.at[1], device_id=(mate, t), device_id_type=MESH,
    )
    hid.start()
    for copy in small:
        copy.wait()
    seg_ref[...] = jnp.broadcast_to(seg_line[...].reshape(1, toks), seg_ref.shape)

    def seg_copy(step, sub):
        at = pl.ds(pl.multiple_of((back - step) * span + core * toks, toks), toks)
        return pltpu.make_async_remote_copy(
            src_ref=seg_ref, dst_ref=segs_ref.at[:, at],
            send_sem=ssend.at[2 * step + sub], recv_sem=srecv.at[2 * step + core],
            device_id=(jnp.minimum(2 * (pair + step) + sub, n_ctx - 1) if step else mate, t),
            device_id_type=MESH,
        )

    for step in range(back + 1):
        if step == 0:
            segs_ref[:, pl.ds(pl.multiple_of(back * span + core * toks, toks), toks)] = seg_ref[...]
            seg_copy(0, 0).start()
        else:
            @pl.when(pair + step < pairs)
            def _():
                seg_copy(step, 0).start()
                seg_copy(step, 1).start()

            @pl.when(pair < step)
            def _():
                rows = slice((back - step) * span, (back - step + 1) * span)
                segs_ref[:, rows] = jnp.full((segs_ref.shape[0], span), -1, jnp.int32)
                kv_ref[:, rows, :] = jnp.zeros((2, span, head), jnp.bfloat16)

    def multiply(d):
        acc = jnp.dot(hbuf[:, :half], wbuf[d, 0], preferred_element_type=jnp.float32)
        return acc + jnp.dot(hbuf[:, half:], wbuf[d, 1], preferred_element_type=jnp.float32)

    def part_copy(d):
        return pltpu.make_async_remote_copy(
            src_ref=part_out.at[d], dst_ref=part_in.at[t],
            send_sem=psend.at[d], recv_sem=precv.at[t],
            device_id=(c, neighbour(d)), device_id_type=MESH,
        )

    def hand_over(d):
        acc = multiply(d)
        part_out[d] = acc.astype(part_out.dtype)

        @pl.when(neighbour(d) == t)
        def _():
            own[...] = acc

        @pl.when(neighbour(d) != t)
        def _():
            part_copy(d).start()

    hid.wait()
    hand_over(0)

    @pl.when(core == 1)
    def _():
        pl.semaphore_wait(gate, 1)
        send_weights()

    x_first.wait_recv()
    relay_y.start()
    y_first.wait_recv()
    relay_x.start()

    angle_rows = (lax.broadcasted_iota(jnp.int32, (span, head), 0) + pair * span).astype(jnp.float32)
    angles = angle_rows * freq_ref[0:1, :]
    is_key = core == 0
    left = lax.broadcasted_iota(jnp.int32, (span, head), 1) < head // 2
    sine = jnp.sin(angles)
    cosb[...] = jnp.where(is_key, jnp.cos(angles), 1.0)
    sinb[...] = jnp.where(is_key, jnp.where(left, -sine, sine), 0.0)

    x_second.wait_recv()
    y_second.wait_recv()

    @pl.when(core == 0)
    def _():
        pl.semaphore_signal(gate, inc=1, device_id=(mate, t), device_id_type=MESH)

    hand_over(1)
    hand_over(2)

    def seg_arrival(step, sub):
        at = pl.ds(pl.multiple_of((back - step) * span + sub * toks, toks), toks)
        return pltpu.make_async_remote_copy(
            src_ref=seg_ref, dst_ref=segs_ref.at[:, at],
            send_sem=ssend.at[0], recv_sem=srecv.at[2 * step + sub],
            device_id=(mate, t), device_id_type=MESH,
        )

    seg_arrival(0, 1 - core).wait_recv()
    for step in range(1, back + 1):
        @pl.when(pair >= step)
        def _():
            seg_arrival(step, 0).wait_recv()
            seg_arrival(step, 1).wait_recv()

    width = halo + toks
    start = pl.multiple_of((core + 2 * back) * toks - halo, toks)
    here = pl.ds(pl.multiple_of((core + 2 * back) * toks, toks), toks)
    key_seg = segs_ref[0:1, pl.ds(start, width)]
    query_seg = jnp.transpose(jnp.broadcast_to(seg_ref[0:1, :], (head, toks)))[:, 0:1]
    row = lax.broadcasted_iota(jnp.int32, (toks, width), 0)
    column = lax.broadcasted_iota(jnp.int32, (toks, width), 1)
    gap = row + halo - column
    allowed = (
        (query_seg == key_seg) & (gap >= 0) & (gap < window_ref[0]) & (column >= halo - c * toks)
    )
    mask[...] = jnp.where(allowed, 0.0, -jnp.inf)

    relay_y.wait_recv()
    relay_x.wait_recv()
    for copy in (x_first, x_second, y_first, y_second, relay_y, relay_x):
        copy.wait_send()

    hand_over(3)

    def kv_copy(kind, src_step, dst_step, send, recv, to):
        return pltpu.make_async_remote_copy(
            src_ref=kv_ref.at[kind, pl.ds((back - src_step) * span, span)],
            dst_ref=kv_ref.at[kind, pl.ds((back - dst_step) * span, span)],
            send_sem=send, recv_sem=recv, device_id=(to, t), device_id_type=MESH,
        )

    def onward(step):
        to = jnp.minimum(2 * (pair + step) + core, n_ctx - 2 + core)
        return kv_copy(core, 0, step, ksend.at[step], krecv.at[step], to)

    def across(step):
        return kv_copy(core, step, step, fsend.at[step], frecv.at[step], mate)

    def crossed(step):
        return kv_copy(1 - core, step, step, fsend.at[step], frecv.at[step], mate)

    def finish(rotated):
        total = own[...] + bias_ref[...].reshape(1, 2 * head)[:, :head].astype(jnp.float32) if rotated else (
            own[...] + bias_ref[...].reshape(1, 2 * head)[:, head:].astype(jnp.float32)
        )
        for step in range(1, n_tp):
            source = (t + step) % n_tp
            pltpu.make_async_remote_copy(
                src_ref=part_out.at[0], dst_ref=part_in.at[source],
                send_sem=psend.at[0], recv_sem=precv.at[source],
                device_id=(c, source), device_id_type=MESH,
            ).wait_recv()
            total = total + part_in[source].astype(jnp.float32)
        if rotated:
            total = total * cosb[...] + pltpu.roll(total, head // 2, 1) * sinb[...]
        kv_ref[0 if rotated else 1, back * span :, :] = total.astype(jnp.bfloat16)
        across(0).start()
        for step in range(1, back + 1):
            @pl.when(pair + step < pairs)
            def _():
                onward(step).start()

    def pass_on():
        for step in range(1, back + 1):
            @pl.when(pair >= step)
            def _():
                onward(step).wait_recv()
                across(step).start()

    def await_crossed():
        crossed(0).wait_recv()
        for step in range(1, back + 1):
            @pl.when(pair >= step)
            def _():
                crossed(step).wait_recv()

    def weigh(lower, upper):
        keys = kv_ref[0, pl.ds(start, width), :]
        scale = head ** (-0.5) * LOG2E

        def one(h):
            lanes = pl.ds(pl.multiple_of(h * head, head), head)
            scores = lax.dot_general(
                q_ref[:, lanes], keys, (((1,), (1,)), ((), ())), preferred_element_type=jnp.float32
            )
            scores = scores + mask[...]
            top = jnp.max(scores, axis=1, keepdims=True)
            weights = jnp.exp2((scores - top) * scale)
            totals[h] = jnp.sum(weights, axis=1, keepdims=True)
            probs[h] = weights.astype(jnp.bfloat16)

        def couple(i, carry):
            one(2 * i)
            one(2 * i + 1)
            return carry

        lax.fori_loop(lower // 2, upper // 2, couple, 0)

    group = q_ref.shape[1] // head
    early = group // 2

    @pl.when(core == 0)
    def _():
        finish(True)
        pass_on()
        weigh(0, group)
        await_crossed()

    @pl.when(core == 1)
    def _():
        await_crossed()
        weigh(0, early)
        finish(False)
        weigh(early, group)
        pass_on()

    values = kv_ref[1, pl.ds(start, width), :]

    def mix(i, carry):
        for h in (2 * i, 2 * i + 1):
            lanes = pl.ds(pl.multiple_of(h * head, head), head)
            mixed = jnp.dot(probs[h], values, preferred_element_type=jnp.float32)
            out_ref[:, lanes] = (mixed / totals[h]).astype(out_ref.dtype)
        return carry

    lax.fori_loop(0, group // 2, mix, 0)
    cache_ref[:, :head] = kv_ref[0, here, :]
    cache_ref[:, head:] = kv_ref[1, here, :]

    for d in range(n_tp):
        @pl.when(neighbour(d) != t)
        def _():
            part_copy(d).wait_send()
    seg_copy(0, 0).wait_send()
    across(0).wait_send()
    for step in range(1, back + 1):
        @pl.when(pair + step < pairs)
        def _():
            seg_copy(step, 0).wait_send()
            seg_copy(step, 1).wait_send()
            onward(step).wait_send()

        @pl.when(pair >= step)
        def _():
            across(step).wait_send()


def fast_body(halo, back, hidden, queries, kv_weight, kv_bias, window, segment_ids):
    toks, feats = hidden.shape
    head = kv_bias.shape[0] // 2
    span = 2 * toks
    group = queries.shape[1] // head
    n_tp = lax.axis_size("tp")
    freqs = rope_base ** (-2.0 * np.arange(head // 2, dtype=np.float64) / head)
    freqs = np.tile(np.concatenate([freqs, freqs])[None, :], (8, 1)).astype(np.float32)
    keys = (back + 1) * span
    vmem = pl.BlockSpec(memory_space=pltpu.VMEM)
    hbm = pl.BlockSpec(memory_space=pl.ANY)
    dma = pltpu.SemaphoreType.DMA
    return pl.pallas_call(
        functools.partial(fused_kernel, halo, back),
        out_shape=(
            pltpu.VMEM(queries.shape, jnp.bfloat16),
            pltpu.VMEM((toks, 2 * head), jnp.bfloat16),
        ),
        in_specs=[pl.BlockSpec(memory_space=pltpu.SMEM), hbm, hbm, hbm, hbm, hbm, hbm],
        out_specs=(vmem, vmem),
        scratch_shapes=[
            pltpu.VMEM((2, keys, head), jnp.bfloat16),
            pltpu.VMEM((8, keys), jnp.int32),
            pltpu.VMEM((span, feats), jnp.bfloat16),
            pltpu.VMEM((n_tp, 2, feats // 2, head), jnp.bfloat16),
            pltpu.VMEM((n_tp, span, head), jnp.bfloat16),
            pltpu.VMEM((n_tp, span, head), jnp.bfloat16),
            pltpu.VMEM((span, head), jnp.float32),
            pltpu.VMEM((span, head), jnp.float32),
            pltpu.VMEM((span, head), jnp.float32),
            pltpu.VMEM(queries.shape, jnp.bfloat16),
            pltpu.VMEM((2 * head,), jnp.bfloat16),
            pltpu.VMEM((8, head), jnp.float32),
            pltpu.VMEM((toks,), jnp.int32),
            pltpu.VMEM((8, toks), jnp.int32),
            pltpu.VMEM((toks, halo + toks), jnp.float32),
            pltpu.VMEM((group, toks, halo + toks), jnp.bfloat16),
            pltpu.VMEM((group, toks, 1), jnp.float32),
            dma((7,)),
            dma((2,)),
            pltpu.SemaphoreType.REGULAR,
            dma((6,)),
            dma((n_tp, 2)),
            dma((n_tp,)),
            dma((n_tp,)),
            dma((back + 1,)),
            dma((back + 1,)),
            dma((back + 1,)),
            dma((back + 1,)),
            dma((2 * back + 2,)),
            dma((2 * back + 2,)),
        ],
        compiler_params=pltpu.CompilerParams(collective_id=0, has_side_effects=True),
    )(window, hidden, kv_weight, queries, kv_bias, jnp.asarray(freqs), segment_ids)


def solution(mesh):
    in_specs = (P("ctx", "tp"), P("ctx", "tp"), P("tp", "ctx"), P("tp"), P("tp"), P("ctx"))
    out_specs = (P("ctx", "tp"), P("ctx", "tp"))
    n_ctx, n_tp = mesh.shape["ctx"], mesh.shape["tp"]

    def step(hidden, queries, kv_weight, kv_bias, window, segment_ids):
        toks = hidden.shape[0]
        args = (hidden, queries, kv_weight, kv_bias, window, segment_ids)
        if n_ctx != 8 or n_ctx != 2 * n_tp or 2 * kv_weight.shape[1] != kv_bias.shape[0]:
            return body(*args)
        longest = min(WINDOW, n_ctx * toks // 2)
        blocks = -(-(longest - 1) // toks)
        return fast_body(blocks * toks, -(-blocks // 2), *args)

    return jax.shard_map(step, mesh=mesh, in_specs=in_specs, out_specs=out_specs, check_vma=False)
```

```python
import functools

import jax
import jax.numpy as jnp
import numpy as np
from jax import lax
from jax.experimental import pallas as pl
from jax.experimental.pallas import tpu as pltpu
from jax.sharding import PartitionSpec as P

WINDOW = 4096
MESH = pl.DeviceIdType.MESH
LOG2E = 1.4426950408889634


rope_base = 1000000.0


def passed_along(value, axis, steps):
    count = lax.axis_size(axis)
    initial, last = (max(0, -steps), min(count, count - steps))
    return lax.ppermute(value, axis, [(source, source + steps) for source in range(initial, last)])


def rotate(values, positions):
    half = values.shape[-1] // 2
    freqs = rope_base ** (-2.0 * jnp.arange(half, dtype=jnp.float32) / values.shape[-1])
    angles = positions.astype(jnp.float32)[:, None] * freqs[None, :]
    cosine = jnp.cos(angles)
    sine = jnp.sin(angles)
    former = values[:, :half]
    latter = values[:, half:]
    return jnp.concatenate(
        [former * cosine - latter * sine, latter * cosine + former * sine], axis=1
    )


def attend(carry, query_rows, query_pos, query_seg, reach, block, block_seg, block_pos):
    running_max, running_sum, weighted = carry
    head = block.shape[1] // 2
    scores = lax.dot_general(
        query_rows, block[:, :head], (((1,), (1,)), ((), ())), preferred_element_type=jnp.float32
    )
    scores = scores * head ** (-0.5)
    gap = query_pos[:, None] - block_pos[None, :]
    allowed = (
        (query_seg[:, None] == block_seg[None, :])
        & (gap >= 0)
        & (gap < reach)
        & (block_pos >= 0)[None, :]
    )
    scores = jnp.where(allowed, scores, -jnp.inf)
    newest = jnp.maximum(running_max, jnp.max(scores, axis=1))
    probs = jnp.exp(scores - newest[:, None])
    rescale = jnp.exp(running_max - newest)
    summed = running_sum * rescale + jnp.sum(probs, axis=1)
    mixed = jnp.dot(probs.astype(jnp.bfloat16), block[:, head:], preferred_element_type=jnp.float32)
    return (newest, summed, weighted * rescale[:, None] + mixed)


def body(hidden, queries, kv_weight, kv_bias, window, segment_ids):
    tok_rows = hidden.shape[0]
    terms = jnp.dot(
        hidden,
        lax.all_gather(kv_weight, "ctx", axis=1, tiled=True),
        preferred_element_type=jnp.float32,
    )
    projected = lax.psum_scatter(terms, "tp", scatter_dimension=1, tiled=True)
    projected = projected + kv_bias.astype(jnp.float32)[None, :]
    head = kv_bias.shape[0] // 2
    shard = lax.axis_index("ctx")
    offsets = jnp.arange(tok_rows, dtype=jnp.int32)
    positions = shard * tok_rows + offsets
    cache = jnp.concatenate(
        [rotate(projected[:, :head], positions), projected[:, head:]], axis=1
    ).astype(jnp.bfloat16)
    group = queries.shape[1] // head
    query_rows = queries.reshape(tok_rows * group, head)
    query_pos = jnp.repeat(positions, group)
    query_seg = jnp.repeat(segment_ids, group)
    reach = window[0]

    def absorb(carry, block, block_seg, block_pos):
        return attend(carry, query_rows, query_pos, query_seg, reach, block, block_seg, block_pos)

    row_count = tok_rows * group
    carry = (
        jnp.full((row_count,), -jnp.inf, jnp.float32),
        jnp.zeros((row_count,), jnp.float32),
        jnp.zeros((row_count, head), jnp.float32),
    )
    carry = absorb(carry, cache, segment_ids, positions)
    halo_count = WINDOW // tok_rows
    held_kv = cache
    held_seg = segment_ids
    have = 0
    while have < halo_count:
        got_kv, got_seg = passed_along((held_kv, held_seg), "ctx", max(have, 1))
        shards = got_kv.shape[0] // tok_rows
        for member in range(shards):
            lower = member * tok_rows
            block_pos = (shard - have - shards + member) * tok_rows + offsets
            carry = absorb(
                carry,
                got_kv[lower : lower + tok_rows],
                got_seg[lower : lower + tok_rows],
                block_pos,
            )
        if have == 0:
            held_kv, held_seg = (got_kv, got_seg)
        else:
            held_kv = jnp.concatenate([got_kv, held_kv], axis=0)
            held_seg = jnp.concatenate([got_seg, held_seg], axis=0)
        have = have + shards
    newest, summed, weighted = carry
    attended = (weighted / summed[:, None]).reshape(tok_rows, group * head).astype(jnp.bfloat16)
    return (attended, cache)


def fused_kernel(
    halo, back, window_ref, hid_hbm, w_hbm, q_hbm, bias_hbm, freq_hbm, seg_hbm,
    probs, totals, near, cache_ref,
    kv_ref, segs_ref, hbuf, wbuf, part_out, part_in, own, cosb, sinb,
    q_ref, bias_ref, freq_ref, seg_line, seg_ref, mask, begun,
    local_sem, hid_sem, gate, clear, wsend, wrecv, relay_recv, psend, precv, ksend, krecv, fsend, frecv, ssend, srecv,
):
    c = lax.axis_index("ctx")
    t = lax.axis_index("tp")
    n_ctx = lax.axis_size("ctx")
    n_tp = lax.axis_size("tp")
    pairs = n_ctx // 2
    pair = c // 2
    core = c % 2
    mate = pair * 2 + (1 - core)
    toks = hid_hbm.shape[0]
    feats, head = w_hbm.shape
    half = feats // 2
    span = 2 * toks
    own_rows = pl.ds(pl.multiple_of(core * toks, toks), toks)

    load_w = [
        pltpu.make_async_copy(w_hbm.at[pl.ds(q * half, half)], wbuf.at[0, q], local_sem.at[q])
        for q in range(2)
    ]
    load_h = pltpu.make_async_copy(hid_hbm, hbuf.at[own_rows], local_sem.at[2])
    small = [
        pltpu.make_async_copy(src, dst, local_sem.at[3 + at])
        for at, (src, dst) in enumerate(
            [(seg_hbm, seg_line), (bias_hbm, bias_ref), (freq_hbm, freq_ref), (q_hbm, q_ref)]
        )
    ]
    load_w[0].start()
    load_w[1].start()
    load_h.start()
    for copy in small:
        copy.start()

    barrier = pltpu.get_barrier_semaphore()
    for step in range(1, n_ctx):
        pl.semaphore_signal(barrier, inc=1, device_id=((c + step) % n_ctx, t), device_id_type=MESH)
    for step in range(1, n_tp):
        pl.semaphore_signal(barrier, inc=1, device_id=(c, (t + step) % n_tp), device_id_type=MESH)
    pl.semaphore_wait(barrier, n_ctx + n_tp - 2)

    def neighbour(d):
        other_x = 1 - pair % 2 if d % 2 else pair % 2
        other_y = 1 - pair // 2 if d // 2 else pair // 2
        return other_y * 2 + other_x

    def w_copy(src, dst, q, to):
        return pltpu.make_async_remote_copy(
            src_ref=wbuf.at[src, q], dst_ref=wbuf.at[dst, q],
            send_sem=wsend, recv_sem=wrecv.at[dst - 1, q],
            device_id=(2 * neighbour(to) + core, t), device_id_type=MESH,
        )

    x_first, x_second = w_copy(0, 1, 0, 1), w_copy(0, 1, 1, 1)
    y_first, y_second = w_copy(0, 2, 1, 2), w_copy(0, 2, 0, 2)
    quarter = half // 2

    def relay_copy(src, q, part, to):
        rows = pl.ds(part * quarter, quarter)
        return pltpu.make_async_remote_copy(
            src_ref=wbuf.at[src, q, rows], dst_ref=wbuf.at[3, q, rows],
            send_sem=wsend, recv_sem=relay_recv.at[q, part],
            device_id=(2 * neighbour(to) + core, t), device_id_type=MESH,
        )

    relay_y = [relay_copy(1, 0, part, 2) for part in range(2)]
    relay_x = [relay_copy(2, 1, part, 1) for part in range(2)]

    def send_weights():
        x_first.start()
        y_first.start()
        x_second.start()
        y_second.start()

    load_w[0].wait()
    load_w[1].wait()

    @pl.when(core == 0)
    def _():
        send_weights()

    load_h.wait()
    hid = pltpu.make_async_remote_copy(
        src_ref=hbuf.at[own_rows], dst_ref=hbuf.at[own_rows],
        send_sem=hid_sem.at[0], recv_sem=hid_sem.at[1], device_id=(mate, t), device_id_type=MESH,
    )
    hid.start()
    for copy in small:
        copy.wait()
    seg_ref[...] = jnp.broadcast_to(seg_line[...].reshape(1, toks), seg_ref.shape)

    def seg_copy(step, sub):
        at = pl.ds(pl.multiple_of((back - step) * span + core * toks, toks), toks)
        return pltpu.make_async_remote_copy(
            src_ref=seg_ref, dst_ref=segs_ref.at[:, at],
            send_sem=ssend.at[2 * step + sub], recv_sem=srecv.at[2 * step + core],
            device_id=(jnp.minimum(2 * (pair + step) + sub, n_ctx - 1) if step else mate, t),
            device_id_type=MESH,
        )

    for step in range(back + 1):
        if step == 0:
            segs_ref[:, pl.ds(pl.multiple_of(back * span + core * toks, toks), toks)] = seg_ref[...]
            seg_copy(0, 0).start()
        else:
            @pl.when(pair + step < pairs)
            def _():
                seg_copy(step, 0).start()
                seg_copy(step, 1).start()

            @pl.when(pair < step)
            def _():
                rows = slice((back - step) * span, (back - step + 1) * span)
                segs_ref[:, rows] = jnp.full((segs_ref.shape[0], span), -1, jnp.int32)
                kv_ref[:, rows, :] = jnp.zeros((2, span, head), jnp.bfloat16)

    low, high = slice(0, toks), slice(toks, span)
    token_halves = (low, high)

    def product(rows, features, weights):
        return jnp.dot(hbuf[rows, features], weights, preferred_element_type=jnp.float32)

    def part_copy(d, r):
        return pltpu.make_async_remote_copy(
            src_ref=part_out.at[d, token_halves[r]], dst_ref=part_in.at[t, token_halves[r]],
            send_sem=psend, recv_sem=precv.at[t, r],
            device_id=(c, neighbour(d)), device_id_type=MESH,
        )

    def hand_over(d, r, acc):
        rows = token_halves[r]
        part_out[d, rows] = acc.astype(part_out.dtype)

        @pl.when(neighbour(d) == t)
        def _():
            own[rows] = acc

        @pl.when(neighbour(d) != t)
        def _():
            part_copy(d, r).start()

    def whole(q):
        return slice(q * half, (q + 1) * half)

    hid.wait()
    every = slice(0, span)
    local = product(every, whole(0), wbuf[0, 0]) + product(every, whole(1), wbuf[0, 1])
    for r in range(2):
        hand_over(0, r, local[token_halves[r]])

    @pl.when(core == 1)
    def _():
        pl.semaphore_wait(gate, 1)
        send_weights()

    x_first.wait_recv()
    for copy in relay_y:
        copy.start()
    y_first.wait_recv()
    for copy in relay_x:
        copy.start()

    angle_rows = (lax.broadcasted_iota(jnp.int32, (span, head), 0) + pair * span).astype(jnp.float32)
    angles = angle_rows * freq_ref[0:1, :]
    is_key = core == 0
    left = lax.broadcasted_iota(jnp.int32, (span, head), 1) < head // 2
    sine = jnp.sin(angles)
    cosb[...] = jnp.where(is_key, jnp.cos(angles), 1.0)
    sinb[...] = jnp.where(is_key, jnp.where(left, -sine, sine), 0.0)

    x_second.wait_recv()
    y_second.wait_recv()

    @pl.when(core == 0)
    def _():
        pl.semaphore_signal(gate, inc=1, device_id=(mate, t), device_id_type=MESH)

    both = sum(
        product(every, whole(q), jnp.concatenate([wbuf[1, q], wbuf[2, q]], axis=1)) for q in range(2)
    )
    for d in (1, 2):
        for r in range(2):
            hand_over(d, r, both[token_halves[r], (d - 1) * head : d * head])
    pltpu.make_async_remote_copy(
        src_ref=wbuf.at[pl.ds(0, 3)], dst_ref=wbuf.at[pl.ds(0, 3)],
        send_sem=wsend, recv_sem=wrecv.at[0, 0], device_id=(mate, t), device_id_type=MESH,
    ).wait_send()

    @pl.when(core == 1)
    def _():
        pl.semaphore_signal(clear, inc=1, device_id=(mate, t), device_id_type=MESH)

    def seg_arrival(step, sub):
        at = pl.ds(pl.multiple_of((back - step) * span + sub * toks, toks), toks)
        return pltpu.make_async_remote_copy(
            src_ref=seg_ref, dst_ref=segs_ref.at[:, at],
            send_sem=ssend.at[0], recv_sem=srecv.at[2 * step + sub],
            device_id=(mate, t), device_id_type=MESH,
        )

    seg_arrival(0, 1 - core).wait_recv()
    for step in range(1, back + 1):
        @pl.when(pair >= step)
        def _():
            seg_arrival(step, 0).wait_recv()
            seg_arrival(step, 1).wait_recv()

    width = halo + toks
    start = pl.multiple_of((core + 2 * back) * toks - halo, toks)
    here = pl.ds(pl.multiple_of((core + 2 * back) * toks, toks), toks)
    key_seg = segs_ref[0:1, pl.ds(start, width)]
    query_seg = jnp.transpose(jnp.broadcast_to(seg_ref[0:1, :], (head, toks)))[:, 0:1]
    row = lax.broadcasted_iota(jnp.int32, (toks, width), 0)
    column = lax.broadcasted_iota(jnp.int32, (toks, width), 1)
    gap = row + halo - column
    allowed = (
        (query_seg == key_seg) & (gap >= 0) & (gap < window_ref[0]) & (column >= halo - c * toks)
    )
    mask[...] = jnp.where(allowed, 0.0, -jnp.inf)

    def far(rows, part):
        return sum(
            product(
                rows, slice(q * half + part * quarter, q * half + (part + 1) * quarter),
                wbuf[3, q, part * quarter : (part + 1) * quarter],
            )
            for q in range(2)
        )

    relay_y[0].wait_recv()
    relay_x[0].wait_recv()
    begun[...] = far(every, 0)
    relay_y[1].wait_recv()
    relay_x[1].wait_recv()
    for r in range(2):
        hand_over(3, r, begun[token_halves[r]] + far(token_halves[r], 1))

    def rows_of(step, r):
        return pl.ds((back - step) * span + r * toks, toks)

    def kv_copy(kind, src_step, dst_step, r, send, recv, to):
        return pltpu.make_async_remote_copy(
            src_ref=kv_ref.at[kind, rows_of(src_step, r)],
            dst_ref=kv_ref.at[kind, rows_of(dst_step, r)],
            send_sem=send.at[dst_step], recv_sem=recv.at[dst_step, r],
            device_id=(to, t), device_id_type=MESH,
        )

    def onward(step, r):
        to = jnp.minimum(2 * (pair + step) + core, n_ctx - 2 + core)
        return kv_copy(core, 0, step, r, ksend, krecv, to)

    def across(step, r):
        return kv_copy(core, step, step, r, fsend, frecv, mate)

    def crossed(step, r):
        return kv_copy(1 - core, step, step, r, fsend, frecv, mate)

    def finish(rotated):
        bias = bias_ref[...].reshape(1, 2 * head).astype(jnp.float32)
        bias = bias[:, :head] if rotated else bias[:, head:]
        for r in range(2):
            rows = token_halves[r]
            total = own[rows] + bias
            for step in range(1, n_tp):
                source = (t + step) % n_tp
                pltpu.make_async_remote_copy(
                    src_ref=part_out.at[0, rows], dst_ref=part_in.at[source, rows],
                    send_sem=psend, recv_sem=precv.at[source, r],
                    device_id=(c, source), device_id_type=MESH,
                ).wait_recv()
                total = total + part_in[source, rows].astype(jnp.float32)
            if rotated:
                total = total * cosb[rows] + pltpu.roll(total, head // 2, 1) * sinb[rows]
            kv_ref[0 if rotated else 1, rows_of(0, r), :] = total.astype(jnp.bfloat16)
            across(0, r).start()
            if rotated and r == 0:
                pl.semaphore_wait(clear, 1)
            for step in range(1, back + 1):
                @pl.when(pair + step < pairs)
                def _():
                    onward(step, r).start()

    def pass_on():
        for r in range(2):
            for step in range(1, back + 1):
                @pl.when(pair >= step)
                def _():
                    onward(step, r).wait_recv()
                    across(step, r).start()

    def await_crossed():
        for step in range(back + 1):
            @pl.when(pair >= step)
            def _():
                for r in range(2):
                    crossed(step, r).wait_recv()

    def weigh(lower, upper):
        keys = kv_ref[0, pl.ds(start, width), :]
        scale = head ** (-0.5) * LOG2E

        def one(h):
            lanes = pl.ds(pl.multiple_of(h * head, head), head)
            scores = lax.dot_general(
                q_ref[:, lanes], keys, (((1,), (1,)), ((), ())), preferred_element_type=jnp.float32
            )
            scores = scores + mask[...]
            top = jnp.max(scores, axis=1, keepdims=True)
            weights = jnp.exp2((scores - top) * scale)
            totals[h] = jnp.sum(weights, axis=1, keepdims=True)
            probs[h] = weights.astype(jnp.bfloat16)

        def couple(i, carry):
            one(2 * i)
            one(2 * i + 1)
            return carry

        lax.fori_loop(lower // 2, upper // 2, couple, 0)

    group = q_ref.shape[1] // head
    early = group // 4 * 2
    behind = pair - (n_tp - 1 - t)
    waits_long = (behind >= 1) & (behind <= back)

    @pl.when(core == 0)
    def _():
        finish(True)
        pass_on()
        weigh(0, group)
        await_crossed()

    @pl.when(core == 1)
    def _():
        finish(False)
        await_crossed()
        weigh(0, early)

        @pl.when(jnp.logical_not(waits_long))
        def _():
            pass_on()

        weigh(early, group)

        @pl.when(waits_long)
        def _():
            pass_on()

    near[...] = kv_ref[1, pl.ds(start, width), :]
    cache_ref[:, :head] = kv_ref[0, here, :]
    cache_ref[:, head:] = kv_ref[1, here, :]

    pltpu.make_async_remote_copy(
        src_ref=part_out.at[pl.ds(0, n_tp - 1)], dst_ref=part_in.at[pl.ds(0, n_tp - 1)],
        send_sem=psend, recv_sem=precv.at[0, 0], device_id=(mate, t), device_id_type=MESH,
    ).wait_send()

    def sent(sem):
        block = kv_ref.at[0, pl.ds(0, span)]
        pltpu.make_async_remote_copy(
            src_ref=block, dst_ref=block, send_sem=sem, recv_sem=krecv.at[0, 0],
            device_id=(mate, t), device_id_type=MESH,
        ).wait_send()

    sent(fsend.at[0])
    seg_copy(0, 0).wait_send()
    for step in range(1, back + 1):
        @pl.when(pair + step < pairs)
        def _():
            sent(ksend.at[step])
            seg_copy(step, 0).wait_send()
            seg_copy(step, 1).wait_send()

        @pl.when(pair >= step)
        def _():
            sent(fsend.at[step])


def mix_kernel(probs, totals, near, cache_ref, out_hbm, cache_hbm, mixed, sems):
    group, _, head = mixed.shape
    cache_copy = pltpu.make_async_copy(cache_ref, cache_hbm, sems.at[group])
    cache_copy.start()

    def out_copy(h):
        lanes = pl.ds(h * head, head)
        return pltpu.make_async_copy(mixed.at[h], out_hbm.at[:, lanes], sems.at[h])

    for h in range(group):
        total = jnp.dot(probs[h], near[...], preferred_element_type=jnp.float32)
        mixed[h] = (total / totals[h]).astype(mixed.dtype)
        out_copy(h).start()
    for h in range(group):
        out_copy(h).wait()
    cache_copy.wait()


def fast_body(halo, back, hidden, queries, kv_weight, kv_bias, window, segment_ids):
    toks, feats = hidden.shape
    head = kv_bias.shape[0] // 2
    span = 2 * toks
    group = queries.shape[1] // head
    n_tp = lax.axis_size("tp")
    freqs = rope_base ** (-2.0 * np.arange(head // 2, dtype=np.float64) / head)
    freqs = np.tile(np.concatenate([freqs, freqs])[None, :], (8, 1)).astype(np.float32)
    keys = (back + 1) * span
    vmem = pl.BlockSpec(memory_space=pltpu.VMEM)
    hbm = pl.BlockSpec(memory_space=pltpu.HBM)
    dma = pltpu.SemaphoreType.DMA
    width = halo + toks
    operands = [
        pltpu.with_memory_space_constraint(array, pltpu.HBM)
        for array in (hidden, kv_weight, queries, kv_bias, jnp.asarray(freqs), segment_ids)
    ]
    made = pl.pallas_call(
        functools.partial(fused_kernel, halo, back),
        out_shape=(
            pltpu.VMEM((group, toks, width), jnp.bfloat16),
            pltpu.VMEM((group, toks, 1), jnp.float32),
            pltpu.VMEM((width, head), jnp.bfloat16),
            pltpu.VMEM((toks, 2 * head), jnp.bfloat16),
        ),
        in_specs=[pl.BlockSpec(memory_space=pltpu.SMEM), hbm, hbm, hbm, hbm, hbm, hbm],
        out_specs=(vmem,) * 4,
        scratch_shapes=[
            pltpu.VMEM((2, keys, head), jnp.bfloat16),
            pltpu.VMEM((8, keys), jnp.int32),
            pltpu.VMEM((span, feats), jnp.bfloat16),
            pltpu.VMEM((n_tp, 2, feats // 2, head), jnp.bfloat16),
            pltpu.VMEM((n_tp, span, head), jnp.bfloat16),
            pltpu.VMEM((n_tp, span, head), jnp.bfloat16),
            pltpu.VMEM((span, head), jnp.float32),
            pltpu.VMEM((span, head), jnp.float32),
            pltpu.VMEM((span, head), jnp.float32),
            pltpu.VMEM(queries.shape, jnp.bfloat16),
            pltpu.VMEM((2 * head,), jnp.bfloat16),
            pltpu.VMEM((8, head), jnp.float32),
            pltpu.VMEM((toks,), jnp.int32),
            pltpu.VMEM((8, toks), jnp.int32),
            pltpu.VMEM((toks, width), jnp.float32),
            pltpu.VMEM((span, head), jnp.float32),
            dma((7,)),
            dma((2,)),
            pltpu.SemaphoreType.REGULAR,
            pltpu.SemaphoreType.REGULAR,
            dma,
            dma((2, 2)),
            dma((2, 2)),
            dma,
            dma((n_tp, 2)),
            dma((back + 1,)),
            dma((back + 1, 2)),
            dma((back + 1,)),
            dma((back + 1, 2)),
            dma((2 * back + 2,)),
            dma((2 * back + 2,)),
        ],
        compiler_params=pltpu.CompilerParams(
            collective_id=0, has_side_effects=True, vmem_limit_bytes=32 << 20
        ),
    )(window, *operands)
    made = [pltpu.with_memory_space_constraint(array, pltpu.VMEM) for array in made]
    return pl.pallas_call(
        mix_kernel,
        out_shape=(
            jax.ShapeDtypeStruct(queries.shape, jnp.bfloat16),
            jax.ShapeDtypeStruct((toks, 2 * head), jnp.bfloat16),
        ),
        in_specs=[vmem] * 4,
        out_specs=(hbm, hbm),
        scratch_shapes=[pltpu.VMEM((group, toks, head), jnp.bfloat16), dma((group + 1,))],
        compiler_params=pltpu.CompilerParams(vmem_limit_bytes=32 << 20),
    )(*made)


def solution(mesh):
    in_specs = (P("ctx", "tp"), P("ctx", "tp"), P("tp", "ctx"), P("tp"), P("tp"), P("ctx"))
    out_specs = (P("ctx", "tp"), P("ctx", "tp"))
    n_ctx, n_tp = mesh.shape["ctx"], mesh.shape["tp"]

    def step(hidden, queries, kv_weight, kv_bias, window, segment_ids):
        toks = hidden.shape[0]
        args = (hidden, queries, kv_weight, kv_bias, window, segment_ids)
        if n_ctx != 8 or n_ctx != 2 * n_tp or 2 * kv_weight.shape[1] != kv_bias.shape[0]:
            return body(*args)
        longest = min(WINDOW, n_ctx * toks // 2)
        blocks = -(-(longest - 1) // toks)
        return fast_body(blocks * toks, -(-blocks // 2), *args)

    return jax.shard_map(step, mesh=mesh, in_specs=in_specs, out_specs=out_specs, check_vma=False)
```

```python
import functools

import jax
import jax.numpy as jnp
import numpy as np
from jax import lax
from jax.experimental import pallas as pl
from jax.experimental.pallas import tpu as pltpu
from jax.sharding import PartitionSpec as P

WINDOW = 4096
MESH = pl.DeviceIdType.MESH
LOG2E = 1.4426950408889634
LOWEST = -1e30


rope_base = 1000000.0


def passed_along(value, axis, steps):
    count = lax.axis_size(axis)
    initial, last = (max(0, -steps), min(count, count - steps))
    return lax.ppermute(value, axis, [(source, source + steps) for source in range(initial, last)])


def rotate(values, positions):
    half = values.shape[-1] // 2
    freqs = rope_base ** (-2.0 * jnp.arange(half, dtype=jnp.float32) / values.shape[-1])
    angles = positions.astype(jnp.float32)[:, None] * freqs[None, :]
    cosine = jnp.cos(angles)
    sine = jnp.sin(angles)
    former = values[:, :half]
    latter = values[:, half:]
    return jnp.concatenate(
        [former * cosine - latter * sine, latter * cosine + former * sine], axis=1
    )


def attend(carry, query_rows, query_pos, query_seg, reach, block, block_seg, block_pos):
    running_max, running_sum, weighted = carry
    head = block.shape[1] // 2
    scores = lax.dot_general(
        query_rows, block[:, :head], (((1,), (1,)), ((), ())), preferred_element_type=jnp.float32
    )
    scores = scores * head ** (-0.5)
    gap = query_pos[:, None] - block_pos[None, :]
    allowed = (
        (query_seg[:, None] == block_seg[None, :])
        & (gap >= 0)
        & (gap < reach)
        & (block_pos >= 0)[None, :]
    )
    scores = jnp.where(allowed, scores, -jnp.inf)
    newest = jnp.maximum(running_max, jnp.max(scores, axis=1))
    probs = jnp.exp(scores - newest[:, None])
    rescale = jnp.exp(running_max - newest)
    summed = running_sum * rescale + jnp.sum(probs, axis=1)
    mixed = jnp.dot(probs.astype(jnp.bfloat16), block[:, head:], preferred_element_type=jnp.float32)
    return (newest, summed, weighted * rescale[:, None] + mixed)


def body(hidden, queries, kv_weight, kv_bias, window, segment_ids):
    tok_rows = hidden.shape[0]
    terms = jnp.dot(
        hidden,
        lax.all_gather(kv_weight, "ctx", axis=1, tiled=True),
        preferred_element_type=jnp.float32,
    )
    projected = lax.psum_scatter(terms, "tp", scatter_dimension=1, tiled=True)
    projected = projected + kv_bias.astype(jnp.float32)[None, :]
    head = kv_bias.shape[0] // 2
    shard = lax.axis_index("ctx")
    offsets = jnp.arange(tok_rows, dtype=jnp.int32)
    positions = shard * tok_rows + offsets
    cache = jnp.concatenate(
        [rotate(projected[:, :head], positions), projected[:, head:]], axis=1
    ).astype(jnp.bfloat16)
    group = queries.shape[1] // head
    query_rows = queries.reshape(tok_rows * group, head)
    query_pos = jnp.repeat(positions, group)
    query_seg = jnp.repeat(segment_ids, group)
    reach = window[0]

    def absorb(carry, block, block_seg, block_pos):
        return attend(carry, query_rows, query_pos, query_seg, reach, block, block_seg, block_pos)

    row_count = tok_rows * group
    carry = (
        jnp.full((row_count,), -jnp.inf, jnp.float32),
        jnp.zeros((row_count,), jnp.float32),
        jnp.zeros((row_count, head), jnp.float32),
    )
    carry = absorb(carry, cache, segment_ids, positions)
    halo_count = WINDOW // tok_rows
    held_kv = cache
    held_seg = segment_ids
    have = 0
    while have < halo_count:
        got_kv, got_seg = passed_along((held_kv, held_seg), "ctx", max(have, 1))
        shards = got_kv.shape[0] // tok_rows
        for member in range(shards):
            lower = member * tok_rows
            block_pos = (shard - have - shards + member) * tok_rows + offsets
            carry = absorb(
                carry,
                got_kv[lower : lower + tok_rows],
                got_seg[lower : lower + tok_rows],
                block_pos,
            )
        if have == 0:
            held_kv, held_seg = (got_kv, got_seg)
        else:
            held_kv = jnp.concatenate([got_kv, held_kv], axis=0)
            held_seg = jnp.concatenate([got_seg, held_seg], axis=0)
        have = have + shards
    newest, summed, weighted = carry
    attended = (weighted / summed[:, None]).reshape(tok_rows, group * head).astype(jnp.bfloat16)
    return (attended, cache)


def fused_kernel(
    halo, back, window_ref, hid_hbm, w_hbm, q_hbm, bias_hbm, freq_hbm, seg_hbm,
    probs, tops, totals, near, cache_ref,
    kv_ref, segs_ref, hbuf, wbuf, part_out, part_in, own, cosb, sinb,
    q_ref, bias_ref, freq_ref, seg_line, seg_ref, mask, begun,
    local_sem, hid_sem, gate, clear, wsend, wrecv, relay_recv, psend, precv, ksend, krecv, fsend, frecv, ssend, srecv,
):
    c = lax.axis_index("ctx")
    t = lax.axis_index("tp")
    n_ctx = lax.axis_size("ctx")
    n_tp = lax.axis_size("tp")
    pairs = n_ctx // 2
    pair = c // 2
    core = c % 2
    mate = pair * 2 + (1 - core)
    toks = hid_hbm.shape[0]
    feats, head = w_hbm.shape
    half = feats // 2
    span = 2 * toks
    own_rows = pl.ds(pl.multiple_of(core * toks, toks), toks)

    load_w = [
        pltpu.make_async_copy(w_hbm.at[pl.ds(q * half, half)], wbuf.at[0, q], local_sem.at[q])
        for q in range(2)
    ]
    load_h = pltpu.make_async_copy(hid_hbm, hbuf.at[own_rows], local_sem.at[2])
    small = [
        pltpu.make_async_copy(src, dst, local_sem.at[3 + at])
        for at, (src, dst) in enumerate(
            [(seg_hbm, seg_line), (bias_hbm, bias_ref), (freq_hbm, freq_ref), (q_hbm, q_ref)]
        )
    ]
    load_w[0].start()
    load_w[1].start()
    load_h.start()
    for copy in small:
        copy.start()

    barrier = pltpu.get_barrier_semaphore()
    for step in range(1, n_ctx):
        pl.semaphore_signal(barrier, inc=1, device_id=((c + step) % n_ctx, t), device_id_type=MESH)
    for step in range(1, n_tp):
        pl.semaphore_signal(barrier, inc=1, device_id=(c, (t + step) % n_tp), device_id_type=MESH)
    pl.semaphore_wait(barrier, n_ctx + n_tp - 2)

    def neighbour(d):
        other_x = 1 - pair % 2 if d % 2 else pair % 2
        other_y = 1 - pair // 2 if d // 2 else pair // 2
        return other_y * 2 + other_x

    def w_copy(src, dst, q, to):
        return pltpu.make_async_remote_copy(
            src_ref=wbuf.at[src, q], dst_ref=wbuf.at[dst, q],
            send_sem=wsend, recv_sem=wrecv.at[dst - 1, q],
            device_id=(2 * neighbour(to) + core, t), device_id_type=MESH,
        )

    x_first, x_second = w_copy(0, 1, 0, 1), w_copy(0, 1, 1, 1)
    y_first, y_second = w_copy(0, 2, 1, 2), w_copy(0, 2, 0, 2)
    quarter = half // 2

    def relay_copy(src, q, part, to):
        rows = pl.ds(part * quarter, quarter)
        return pltpu.make_async_remote_copy(
            src_ref=wbuf.at[src, q, rows], dst_ref=wbuf.at[3, q, rows],
            send_sem=wsend, recv_sem=relay_recv.at[q, part],
            device_id=(2 * neighbour(to) + core, t), device_id_type=MESH,
        )

    relay_y = [relay_copy(1, 0, part, 2) for part in range(2)]
    relay_x = [relay_copy(2, 1, part, 1) for part in range(2)]

    def send_weights():
        x_first.start()
        y_first.start()
        x_second.start()
        y_second.start()

    load_w[0].wait()
    load_w[1].wait()

    @pl.when(core == 0)
    def _():
        send_weights()

    load_h.wait()
    hid = pltpu.make_async_remote_copy(
        src_ref=hbuf.at[own_rows], dst_ref=hbuf.at[own_rows],
        send_sem=hid_sem.at[0], recv_sem=hid_sem.at[1], device_id=(mate, t), device_id_type=MESH,
    )
    hid.start()
    for copy in small:
        copy.wait()
    seg_ref[...] = jnp.broadcast_to(seg_line[...].reshape(1, toks), seg_ref.shape)

    def seg_copy(step, sub):
        at = pl.ds(pl.multiple_of((back - step) * span + core * toks, toks), toks)
        return pltpu.make_async_remote_copy(
            src_ref=seg_ref, dst_ref=segs_ref.at[:, at],
            send_sem=ssend.at[2 * step + sub], recv_sem=srecv.at[2 * step + core],
            device_id=(jnp.minimum(2 * (pair + step) + sub, n_ctx - 1) if step else mate, t),
            device_id_type=MESH,
        )

    for step in range(back + 1):
        if step == 0:
            segs_ref[:, pl.ds(pl.multiple_of(back * span + core * toks, toks), toks)] = seg_ref[...]
            seg_copy(0, 0).start()
        else:
            @pl.when(pair + step < pairs)
            def _():
                seg_copy(step, 0).start()
                seg_copy(step, 1).start()

            @pl.when(pair < step)
            def _():
                rows = slice((back - step) * span, (back - step + 1) * span)
                segs_ref[:, rows] = jnp.full((segs_ref.shape[0], span), -1, jnp.int32)
                kv_ref[:, rows, :] = jnp.zeros((2, span, head), jnp.bfloat16)

    low, high = slice(0, toks), slice(toks, span)
    token_halves = (low, high)

    def product(rows, features, weights):
        return jnp.dot(hbuf[rows, features], weights, preferred_element_type=jnp.float32)

    def part_copy(d, r):
        return pltpu.make_async_remote_copy(
            src_ref=part_out.at[d, token_halves[r]], dst_ref=part_in.at[t, token_halves[r]],
            send_sem=psend, recv_sem=precv.at[t, r],
            device_id=(c, neighbour(d)), device_id_type=MESH,
        )

    def hand_over(d, r, acc):
        rows = token_halves[r]
        part_out[d, rows] = acc.astype(part_out.dtype)

        @pl.when(neighbour(d) == t)
        def _():
            own[rows] = acc

        @pl.when(neighbour(d) != t)
        def _():
            part_copy(d, r).start()

    def whole(q):
        return slice(q * half, (q + 1) * half)

    hid.wait()
    every = slice(0, span)
    local = product(every, whole(0), wbuf[0, 0]) + product(every, whole(1), wbuf[0, 1])
    for r in range(2):
        hand_over(0, r, local[token_halves[r]])

    @pl.when(core == 1)
    def _():
        pl.semaphore_wait(gate, 1)
        send_weights()

    x_first.wait_recv()
    for copy in relay_y:
        copy.start()
    y_first.wait_recv()
    for copy in relay_x:
        copy.start()

    angle_rows = (lax.broadcasted_iota(jnp.int32, (span, head), 0) + pair * span).astype(jnp.float32)
    angles = angle_rows * freq_ref[0:1, :]
    is_key = core == 0
    left = lax.broadcasted_iota(jnp.int32, (span, head), 1) < head // 2
    sine = jnp.sin(angles)
    cosb[...] = jnp.where(is_key, jnp.cos(angles), 1.0)
    sinb[...] = jnp.where(is_key, jnp.where(left, -sine, sine), 0.0)

    x_second.wait_recv()
    y_second.wait_recv()

    @pl.when(core == 0)
    def _():
        pl.semaphore_signal(gate, inc=1, device_id=(mate, t), device_id_type=MESH)

    both = sum(
        product(every, whole(q), jnp.concatenate([wbuf[1, q], wbuf[2, q]], axis=1)) for q in range(2)
    )
    for d in (1, 2):
        for r in range(2):
            hand_over(d, r, both[token_halves[r], (d - 1) * head : d * head])
    pltpu.make_async_remote_copy(
        src_ref=wbuf.at[pl.ds(0, 3)], dst_ref=wbuf.at[pl.ds(0, 3)],
        send_sem=wsend, recv_sem=wrecv.at[0, 0], device_id=(mate, t), device_id_type=MESH,
    ).wait_send()

    @pl.when(core == 1)
    def _():
        pl.semaphore_signal(clear, inc=1, device_id=(mate, t), device_id_type=MESH)

    def seg_arrival(step, sub):
        at = pl.ds(pl.multiple_of((back - step) * span + sub * toks, toks), toks)
        return pltpu.make_async_remote_copy(
            src_ref=seg_ref, dst_ref=segs_ref.at[:, at],
            send_sem=ssend.at[0], recv_sem=srecv.at[2 * step + sub],
            device_id=(mate, t), device_id_type=MESH,
        )

    seg_arrival(0, 1 - core).wait_recv()
    for step in range(1, back + 1):
        @pl.when(pair >= step)
        def _():
            seg_arrival(step, 0).wait_recv()
            seg_arrival(step, 1).wait_recv()

    width = halo + toks
    start = pl.multiple_of((core + 2 * back) * toks - halo, toks)
    here = pl.ds(pl.multiple_of((core + 2 * back) * toks, toks), toks)
    key_seg = segs_ref[0:1, pl.ds(start, width)]
    query_seg = jnp.transpose(jnp.broadcast_to(seg_ref[0:1, :], (head, toks)))[:, 0:1]
    row = lax.broadcasted_iota(jnp.int32, (toks, width), 0)
    column = lax.broadcasted_iota(jnp.int32, (toks, width), 1)
    gap = row + halo - column
    allowed = (
        (query_seg == key_seg) & (gap >= 0) & (gap < window_ref[0]) & (column >= halo - c * toks)
    )
    mask[...] = jnp.where(allowed, 0.0, -jnp.inf)

    def far(rows, part):
        return sum(
            product(
                rows, slice(q * half + part * quarter, q * half + (part + 1) * quarter),
                wbuf[3, q, part * quarter : (part + 1) * quarter],
            )
            for q in range(2)
        )

    relay_y[0].wait_recv()
    relay_x[0].wait_recv()
    begun[...] = far(every, 0)
    relay_y[1].wait_recv()
    relay_x[1].wait_recv()
    for r in range(2):
        hand_over(3, r, begun[token_halves[r]] + far(token_halves[r], 1))

    def rows_of(step, r):
        return pl.ds((back - step) * span + r * toks, toks)

    def kv_copy(kind, src_step, dst_step, r, send, recv, to):
        return pltpu.make_async_remote_copy(
            src_ref=kv_ref.at[kind, rows_of(src_step, r)],
            dst_ref=kv_ref.at[kind, rows_of(dst_step, r)],
            send_sem=send.at[dst_step], recv_sem=recv.at[dst_step, r],
            device_id=(to, t), device_id_type=MESH,
        )

    def onward(step, r):
        to = jnp.minimum(2 * (pair + step) + core, n_ctx - 2 + core)
        return kv_copy(core, 0, step, r, ksend, krecv, to)

    def across(step, r):
        return kv_copy(core, step, step, r, fsend, frecv, mate)

    def crossed(step, r):
        return kv_copy(1 - core, step, step, r, fsend, frecv, mate)

    def finish(rotated):
        bias = bias_ref[...].reshape(1, 2 * head).astype(jnp.float32)
        bias = bias[:, :head] if rotated else bias[:, head:]
        for r in range(2):
            rows = token_halves[r]
            total = own[rows] + bias
            for step in range(1, n_tp):
                source = (t + step) % n_tp
                pltpu.make_async_remote_copy(
                    src_ref=part_out.at[0, rows], dst_ref=part_in.at[source, rows],
                    send_sem=psend, recv_sem=precv.at[source, r],
                    device_id=(c, source), device_id_type=MESH,
                ).wait_recv()
                total = total + part_in[source, rows].astype(jnp.float32)
            if rotated:
                total = total * cosb[rows] + pltpu.roll(total, head // 2, 1) * sinb[rows]
            kv_ref[0 if rotated else 1, rows_of(0, r), :] = total.astype(jnp.bfloat16)
            across(0, r).start()
            if rotated and r == 0:
                pl.semaphore_wait(clear, 1)
            for step in range(1, back + 1):
                @pl.when(pair + step < pairs)
                def _():
                    onward(step, r).start()

    def pass_on():
        for r in range(2):
            for step in range(1, back + 1):
                @pl.when(pair >= step)
                def _():
                    onward(step, r).wait_recv()
                    across(step, r).start()

    def await_crossed(steps):
        for step in steps:
            @pl.when(pair >= step)
            def _():
                for r in range(2):
                    crossed(step, r).wait_recv()

    def weigh(part, first, last, lower, upper):
        keys = kv_ref[0, pl.ds(pl.multiple_of(start + first, toks), last - first), :]
        scale = head ** (-0.5) * LOG2E

        def one(h):
            lanes = pl.ds(pl.multiple_of(h * head, head), head)
            scores = lax.dot_general(
                q_ref[:, lanes], keys, (((1,), (1,)), ((), ())), preferred_element_type=jnp.float32
            )
            scores = scores + mask[:, first:last]
            top = jnp.maximum(jnp.max(scores, axis=1, keepdims=True), LOWEST)
            weights = jnp.exp2((scores - top) * scale)
            tops[part, h] = top
            totals[part, h] = jnp.sum(weights, axis=1, keepdims=True)
            probs[h, :, first:last] = weights.astype(jnp.bfloat16)

        def couple(i, carry):
            one(2 * i)
            one(2 * i + 1)
            return carry

        lax.fori_loop(lower // 2, upper // 2, couple, 0)

    group = q_ref.shape[1] // head
    early = group // 4 * 2
    behind = pair - (n_tp - 1 - t)
    waits_long = (behind >= 1) & (behind <= back)

    @pl.when(core == 0)
    def _():
        finish(True)
        weigh(0, halo, width, 0, group)
        pass_on()
        weigh(1, 0, halo, 0, group)
        await_crossed(range(back + 1))

    @pl.when(core == 1)
    def _():
        split = halo - toks
        await_crossed([0])
        weigh(0, split, width, 0, group)
        finish(False)
        await_crossed(range(1, back + 1))
        weigh(1, 0, split, 0, early)

        @pl.when(jnp.logical_not(waits_long))
        def _():
            pass_on()

        weigh(1, 0, split, early, group)

        @pl.when(waits_long)
        def _():
            pass_on()

    near[...] = kv_ref[1, pl.ds(start, width), :]
    cache_ref[:, :head] = kv_ref[0, here, :]
    cache_ref[:, head:] = kv_ref[1, here, :]

    pltpu.make_async_remote_copy(
        src_ref=part_out.at[pl.ds(0, n_tp - 1)], dst_ref=part_in.at[pl.ds(0, n_tp - 1)],
        send_sem=psend, recv_sem=precv.at[0, 0], device_id=(mate, t), device_id_type=MESH,
    ).wait_send()

    def sent(sem):
        block = kv_ref.at[0, pl.ds(0, span)]
        pltpu.make_async_remote_copy(
            src_ref=block, dst_ref=block, send_sem=sem, recv_sem=krecv.at[0, 0],
            device_id=(mate, t), device_id_type=MESH,
        ).wait_send()

    sent(fsend.at[0])
    seg_copy(0, 0).wait_send()
    for step in range(1, back + 1):
        @pl.when(pair + step < pairs)
        def _():
            sent(ksend.at[step])
            seg_copy(step, 0).wait_send()
            seg_copy(step, 1).wait_send()

        @pl.when(pair >= step)
        def _():
            sent(fsend.at[step])


def mix_kernel(probs, tops, totals, near, cache_ref, out_hbm, cache_hbm, mixed, sems):
    group, toks, head = mixed.shape
    width = near.shape[0]
    scale = head ** (-0.5) * LOG2E
    cache_copy = pltpu.make_async_copy(cache_ref, cache_hbm, sems.at[group])
    cache_copy.start()

    def out_copy(h):
        lanes = pl.ds(h * head, head)
        return pltpu.make_async_copy(mixed.at[h], out_hbm.at[:, lanes], sems.at[h])

    def mix(split):
        for h in range(group):
            highest = jnp.maximum(tops[0, h], tops[1, h])
            lift = [jnp.exp2((tops[part, h] - highest) * scale) for part in range(2)]
            total = lift[0] * totals[0, h] + lift[1] * totals[1, h]
            own = jnp.dot(probs[h, :, split:], near[split:], preferred_element_type=jnp.float32)
            far = jnp.dot(probs[h, :, :split], near[:split], preferred_element_type=jnp.float32)
            mixed[h] = (own * (lift[0] / total) + far * (lift[1] / total)).astype(mixed.dtype)
            out_copy(h).start()

    core = lax.axis_index("ctx") % 2

    @pl.when(core == 0)
    def _():
        mix(width - toks)

    @pl.when(core == 1)
    def _():
        mix(width - 2 * toks)

    for h in range(group):
        out_copy(h).wait()
    cache_copy.wait()


def fast_body(halo, back, hidden, queries, kv_weight, kv_bias, window, segment_ids):
    toks, feats = hidden.shape
    head = kv_bias.shape[0] // 2
    span = 2 * toks
    group = queries.shape[1] // head
    n_tp = lax.axis_size("tp")
    freqs = rope_base ** (-2.0 * np.arange(head // 2, dtype=np.float64) / head)
    freqs = np.tile(np.concatenate([freqs, freqs])[None, :], (8, 1)).astype(np.float32)
    keys = (back + 1) * span
    vmem = pl.BlockSpec(memory_space=pltpu.VMEM)
    hbm = pl.BlockSpec(memory_space=pltpu.HBM)
    dma = pltpu.SemaphoreType.DMA
    width = halo + toks
    operands = [
        pltpu.with_memory_space_constraint(array, pltpu.HBM)
        for array in (hidden, kv_weight, queries, kv_bias, jnp.asarray(freqs), segment_ids)
    ]
    made = pl.pallas_call(
        functools.partial(fused_kernel, halo, back),
        out_shape=(
            pltpu.VMEM((group, toks, width), jnp.bfloat16),
            pltpu.VMEM((2, group, toks, 1), jnp.float32),
            pltpu.VMEM((2, group, toks, 1), jnp.float32),
            pltpu.VMEM((width, head), jnp.bfloat16),
            pltpu.VMEM((toks, 2 * head), jnp.bfloat16),
        ),
        in_specs=[pl.BlockSpec(memory_space=pltpu.SMEM), hbm, hbm, hbm, hbm, hbm, hbm],
        out_specs=(vmem,) * 5,
        scratch_shapes=[
            pltpu.VMEM((2, keys, head), jnp.bfloat16),
            pltpu.VMEM((8, keys), jnp.int32),
            pltpu.VMEM((span, feats), jnp.bfloat16),
            pltpu.VMEM((n_tp, 2, feats // 2, head), jnp.bfloat16),
            pltpu.VMEM((n_tp, span, head), jnp.bfloat16),
            pltpu.VMEM((n_tp, span, head), jnp.bfloat16),
            pltpu.VMEM((span, head), jnp.float32),
            pltpu.VMEM((span, head), jnp.float32),
            pltpu.VMEM((span, head), jnp.float32),
            pltpu.VMEM(queries.shape, jnp.bfloat16),
            pltpu.VMEM((2 * head,), jnp.bfloat16),
            pltpu.VMEM((8, head), jnp.float32),
            pltpu.VMEM((toks,), jnp.int32),
            pltpu.VMEM((8, toks), jnp.int32),
            pltpu.VMEM((toks, width), jnp.float32),
            pltpu.VMEM((span, head), jnp.float32),
            dma((7,)),
            dma((2,)),
            pltpu.SemaphoreType.REGULAR,
            pltpu.SemaphoreType.REGULAR,
            dma,
            dma((2, 2)),
            dma((2, 2)),
            dma,
            dma((n_tp, 2)),
            dma((back + 1,)),
            dma((back + 1, 2)),
            dma((back + 1,)),
            dma((back + 1, 2)),
            dma((2 * back + 2,)),
            dma((2 * back + 2,)),
        ],
        compiler_params=pltpu.CompilerParams(
            collective_id=0, has_side_effects=True, vmem_limit_bytes=32 << 20
        ),
    )(window, *operands)
    made = [pltpu.with_memory_space_constraint(array, pltpu.VMEM) for array in made]
    return pl.pallas_call(
        mix_kernel,
        out_shape=(
            jax.ShapeDtypeStruct(queries.shape, jnp.bfloat16),
            jax.ShapeDtypeStruct((toks, 2 * head), jnp.bfloat16),
        ),
        in_specs=[vmem] * 5,
        out_specs=(hbm, hbm),
        scratch_shapes=[pltpu.VMEM((group, toks, head), jnp.bfloat16), dma((group + 1,))],
        compiler_params=pltpu.CompilerParams(vmem_limit_bytes=32 << 20),
    )(*made)


def solution(mesh):
    in_specs = (P("ctx", "tp"), P("ctx", "tp"), P("tp", "ctx"), P("tp"), P("tp"), P("ctx"))
    out_specs = (P("ctx", "tp"), P("ctx", "tp"))
    n_ctx, n_tp = mesh.shape["ctx"], mesh.shape["tp"]

    def step(hidden, queries, kv_weight, kv_bias, window, segment_ids):
        toks = hidden.shape[0]
        args = (hidden, queries, kv_weight, kv_bias, window, segment_ids)
        if n_ctx != 8 or n_ctx != 2 * n_tp or 2 * kv_weight.shape[1] != kv_bias.shape[0]:
            return body(*args)
        longest = min(WINDOW, n_ctx * toks // 2)
        blocks = -(-(longest - 1) // toks)
        return fast_body(blocks * toks, -(-blocks // 2), *args)

    return jax.shard_map(step, mesh=mesh, in_specs=in_specs, out_specs=out_specs, check_vma=False)
```

```python
import functools

import jax
import jax.numpy as jnp
import numpy as np
from jax import lax
from jax.experimental import pallas as pl
from jax.experimental.pallas import tpu as pltpu
from jax.sharding import PartitionSpec as P

WINDOW = 4096
MESH = pl.DeviceIdType.MESH
LOG2E = 1.4426950408889634
LOWEST = -1e30


rope_base = 1000000.0


def passed_along(value, axis, steps):
    count = lax.axis_size(axis)
    initial, last = (max(0, -steps), min(count, count - steps))
    return lax.ppermute(value, axis, [(source, source + steps) for source in range(initial, last)])


def rotate(values, positions):
    half = values.shape[-1] // 2
    freqs = rope_base ** (-2.0 * jnp.arange(half, dtype=jnp.float32) / values.shape[-1])
    angles = positions.astype(jnp.float32)[:, None] * freqs[None, :]
    cosine = jnp.cos(angles)
    sine = jnp.sin(angles)
    former = values[:, :half]
    latter = values[:, half:]
    return jnp.concatenate(
        [former * cosine - latter * sine, latter * cosine + former * sine], axis=1
    )


def attend(carry, query_rows, query_pos, query_seg, reach, block, block_seg, block_pos):
    running_max, running_sum, weighted = carry
    head = block.shape[1] // 2
    scores = lax.dot_general(
        query_rows, block[:, :head], (((1,), (1,)), ((), ())), preferred_element_type=jnp.float32
    )
    scores = scores * head ** (-0.5)
    gap = query_pos[:, None] - block_pos[None, :]
    allowed = (
        (query_seg[:, None] == block_seg[None, :])
        & (gap >= 0)
        & (gap < reach)
        & (block_pos >= 0)[None, :]
    )
    scores = jnp.where(allowed, scores, -jnp.inf)
    newest = jnp.maximum(running_max, jnp.max(scores, axis=1))
    probs = jnp.exp(scores - newest[:, None])
    rescale = jnp.exp(running_max - newest)
    summed = running_sum * rescale + jnp.sum(probs, axis=1)
    mixed = jnp.dot(probs.astype(jnp.bfloat16), block[:, head:], preferred_element_type=jnp.float32)
    return (newest, summed, weighted * rescale[:, None] + mixed)


def body(hidden, queries, kv_weight, kv_bias, window, segment_ids):
    tok_rows = hidden.shape[0]
    terms = jnp.dot(
        hidden,
        lax.all_gather(kv_weight, "ctx", axis=1, tiled=True),
        preferred_element_type=jnp.float32,
    )
    projected = lax.psum_scatter(terms, "tp", scatter_dimension=1, tiled=True)
    projected = projected + kv_bias.astype(jnp.float32)[None, :]
    head = kv_bias.shape[0] // 2
    shard = lax.axis_index("ctx")
    offsets = jnp.arange(tok_rows, dtype=jnp.int32)
    positions = shard * tok_rows + offsets
    cache = jnp.concatenate(
        [rotate(projected[:, :head], positions), projected[:, head:]], axis=1
    ).astype(jnp.bfloat16)
    group = queries.shape[1] // head
    query_rows = queries.reshape(tok_rows * group, head)
    query_pos = jnp.repeat(positions, group)
    query_seg = jnp.repeat(segment_ids, group)
    reach = window[0]

    def absorb(carry, block, block_seg, block_pos):
        return attend(carry, query_rows, query_pos, query_seg, reach, block, block_seg, block_pos)

    row_count = tok_rows * group
    carry = (
        jnp.full((row_count,), -jnp.inf, jnp.float32),
        jnp.zeros((row_count,), jnp.float32),
        jnp.zeros((row_count, head), jnp.float32),
    )
    carry = absorb(carry, cache, segment_ids, positions)
    halo_count = WINDOW // tok_rows
    held_kv = cache
    held_seg = segment_ids
    have = 0
    while have < halo_count:
        got_kv, got_seg = passed_along((held_kv, held_seg), "ctx", max(have, 1))
        shards = got_kv.shape[0] // tok_rows
        for member in range(shards):
            lower = member * tok_rows
            block_pos = (shard - have - shards + member) * tok_rows + offsets
            carry = absorb(
                carry,
                got_kv[lower : lower + tok_rows],
                got_seg[lower : lower + tok_rows],
                block_pos,
            )
        if have == 0:
            held_kv, held_seg = (got_kv, got_seg)
        else:
            held_kv = jnp.concatenate([got_kv, held_kv], axis=0)
            held_seg = jnp.concatenate([got_seg, held_seg], axis=0)
        have = have + shards
    newest, summed, weighted = carry
    attended = (weighted / summed[:, None]).reshape(tok_rows, group * head).astype(jnp.bfloat16)
    return (attended, cache)


def fused_kernel(
    halo, back, window_ref, hid_hbm, w_hbm, q_hbm, bias_hbm, freq_hbm, seg_hbm,
    probs, tops, base, near, cache_ref,
    kv_ref, segs_ref, hbuf, wbuf, part_out, part_in, own, cosb, sinb,
    q_ref, bias_ref, freq_ref, seg_line, seg_ref, mask, begun,
    local_sem, hid_sem, gate, clear, wsend, wrecv, relay_recv, psend, precv, ksend, krecv, fsend, frecv, ssend, srecv,
):
    c = lax.axis_index("ctx")
    t = lax.axis_index("tp")
    n_ctx = lax.axis_size("ctx")
    n_tp = lax.axis_size("tp")
    pairs = n_ctx // 2
    pair = c // 2
    core = c % 2
    mate = pair * 2 + (1 - core)
    toks = hid_hbm.shape[0]
    feats, head = w_hbm.shape
    half = feats // 2
    span = 2 * toks
    own_rows = pl.ds(pl.multiple_of(core * toks, toks), toks)

    load_w = [
        pltpu.make_async_copy(w_hbm.at[pl.ds(q * half, half)], wbuf.at[0, q], local_sem.at[q])
        for q in range(2)
    ]
    load_h = pltpu.make_async_copy(hid_hbm, hbuf.at[own_rows], local_sem.at[2])
    small = [
        pltpu.make_async_copy(src, dst, local_sem.at[3 + at])
        for at, (src, dst) in enumerate(
            [(seg_hbm, seg_line), (bias_hbm, bias_ref), (freq_hbm, freq_ref), (q_hbm, q_ref)]
        )
    ]
    load_w[0].start()
    load_w[1].start()
    load_h.start()
    for copy in small:
        copy.start()

    barrier = pltpu.get_barrier_semaphore()
    for step in range(1, n_ctx):
        pl.semaphore_signal(barrier, inc=1, device_id=((c + step) % n_ctx, t), device_id_type=MESH)
    for step in range(1, n_tp):
        pl.semaphore_signal(barrier, inc=1, device_id=(c, (t + step) % n_tp), device_id_type=MESH)
    pl.semaphore_wait(barrier, n_ctx + n_tp - 2)

    def neighbour(d):
        other_x = 1 - pair % 2 if d % 2 else pair % 2
        other_y = 1 - pair // 2 if d // 2 else pair // 2
        return other_y * 2 + other_x

    def w_copy(src, dst, q, to):
        return pltpu.make_async_remote_copy(
            src_ref=wbuf.at[src, q], dst_ref=wbuf.at[dst, q],
            send_sem=wsend, recv_sem=wrecv.at[dst - 1, q],
            device_id=(2 * neighbour(to) + core, t), device_id_type=MESH,
        )

    x_first, x_second = w_copy(0, 1, 0, 1), w_copy(0, 1, 1, 1)
    y_first, y_second = w_copy(0, 2, 1, 2), w_copy(0, 2, 0, 2)
    quarter = half // 2

    def relay_copy(src, q, part, to):
        rows = pl.ds(part * quarter, quarter)
        return pltpu.make_async_remote_copy(
            src_ref=wbuf.at[src, q, rows], dst_ref=wbuf.at[3, q, rows],
            send_sem=wsend, recv_sem=relay_recv.at[part],
            device_id=(2 * neighbour(to) + core, t), device_id_type=MESH,
        )

    relay_y = [relay_copy(1, 0, part, 2) for part in range(2)]
    relay_x = [relay_copy(2, 1, part, 1) for part in range(2)]

    def send_weights():
        x_first.start()
        y_first.start()
        x_second.start()
        y_second.start()

    load_w[0].wait()
    load_w[1].wait()

    @pl.when(core == 0)
    def _():
        send_weights()

    load_h.wait()
    hid = pltpu.make_async_remote_copy(
        src_ref=hbuf.at[own_rows], dst_ref=hbuf.at[own_rows],
        send_sem=hid_sem.at[0], recv_sem=hid_sem.at[1], device_id=(mate, t), device_id_type=MESH,
    )
    hid.start()
    for copy in small:
        copy.wait()
    seg_ref[...] = jnp.broadcast_to(seg_line[...].reshape(1, toks), seg_ref.shape)

    def seg_copy(step, sub):
        at = pl.ds(pl.multiple_of((back - step) * span + core * toks, toks), toks)
        return pltpu.make_async_remote_copy(
            src_ref=seg_ref, dst_ref=segs_ref.at[:, at],
            send_sem=ssend.at[step], recv_sem=srecv.at[step],
            device_id=(jnp.minimum(2 * (pair + step) + sub, n_ctx - 1) if step else mate, t),
            device_id_type=MESH,
        )

    for step in range(back + 1):
        if step == 0:
            segs_ref[:, pl.ds(pl.multiple_of(back * span + core * toks, toks), toks)] = seg_ref[...]
            seg_copy(0, 0).start()
        else:
            @pl.when(pair + step < pairs)
            def _():
                seg_copy(step, 0).start()
                seg_copy(step, 1).start()

            @pl.when(pair < step)
            def _():
                rows = slice((back - step) * span, (back - step + 1) * span)
                segs_ref[:, rows] = jnp.full((segs_ref.shape[0], span), -1, jnp.int32)
                kv_ref[:, rows, :] = jnp.zeros((2, span, head), jnp.bfloat16)

    low, high = slice(0, toks), slice(toks, span)
    token_halves = (low, high)

    def product(rows, features, weights):
        return jnp.dot(hbuf[rows, features], weights, preferred_element_type=jnp.float32)

    def part_copy(d, r):
        return pltpu.make_async_remote_copy(
            src_ref=part_out.at[d, token_halves[r]], dst_ref=part_in.at[t, token_halves[r]],
            send_sem=psend, recv_sem=precv.at[(t - neighbour(d) + n_tp - 1) % n_tp, r],
            device_id=(c, neighbour(d)), device_id_type=MESH,
        )

    def hand_over(d, r, acc):
        rows = token_halves[r]
        part_out[d, rows] = acc.astype(part_out.dtype)

        @pl.when(neighbour(d) == t)
        def _():
            own[rows] = acc

        @pl.when(neighbour(d) != t)
        def _():
            part_copy(d, r).start()

    def whole(q):
        return slice(q * half, (q + 1) * half)

    hid.wait()
    every = slice(0, span)
    local = product(every, whole(0), wbuf[0, 0]) + product(every, whole(1), wbuf[0, 1])
    for r in range(2):
        hand_over(0, r, local[token_halves[r]])

    @pl.when(core == 1)
    def _():
        pl.semaphore_wait(gate, 1)
        send_weights()

    x_first.wait_recv()
    for copy in relay_y:
        copy.start()
    y_first.wait_recv()
    for copy in relay_x:
        copy.start()

    angle_rows = (lax.broadcasted_iota(jnp.int32, (span, head), 0) + pair * span).astype(jnp.float32)
    angles = angle_rows * freq_ref[0:1, :]
    is_key = core == 0
    left = lax.broadcasted_iota(jnp.int32, (span, head), 1) < head // 2
    sine = jnp.sin(angles)
    cosb[...] = jnp.where(is_key, jnp.cos(angles), 1.0)
    sinb[...] = jnp.where(is_key, jnp.where(left, -sine, sine), 0.0)

    for d in (1, 2):
        begun[d - 1] = product(every, whole(d - 1), wbuf[d, d - 1])
    y_second.wait_recv()
    x_second.wait_recv()

    @pl.when(core == 0)
    def _():
        pl.semaphore_signal(gate, inc=1, device_id=(mate, t), device_id_type=MESH)

    for d in (2, 1):
        full = begun[d - 1] + product(every, whole(2 - d), wbuf[d, 2 - d])
        for r in range(2):
            hand_over(d, r, full[token_halves[r]])
    pltpu.make_async_remote_copy(
        src_ref=wbuf.at[pl.ds(0, 3)], dst_ref=wbuf.at[pl.ds(0, 3)],
        send_sem=wsend, recv_sem=wrecv.at[0, 0], device_id=(mate, t), device_id_type=MESH,
    ).wait_send()

    @pl.when(core == 1)
    def _():
        pl.semaphore_signal(clear, inc=1, device_id=(mate, t), device_id_type=MESH)

    def seg_block(step, count):
        block = segs_ref.at[:, pl.ds((back - step) * span, count * toks)]
        return pltpu.make_async_remote_copy(
            src_ref=block, dst_ref=block, send_sem=ssend.at[step], recv_sem=srecv.at[step],
            device_id=(mate, t), device_id_type=MESH,
        )

    seg_block(0, 1).wait_recv()
    for step in range(1, back + 1):
        @pl.when(pair >= step)
        def _():
            seg_block(step, 2).wait_recv()

    width = halo + toks
    start = pl.multiple_of((core + 2 * back) * toks - halo, toks)
    here = pl.ds(pl.multiple_of((core + 2 * back) * toks, toks), toks)
    key_seg = segs_ref[0:1, pl.ds(start, width)]
    query_seg = jnp.transpose(jnp.broadcast_to(seg_ref[0:1, :], (head, toks)))[:, 0:1]
    row = lax.broadcasted_iota(jnp.int32, (toks, width), 0)
    column = lax.broadcasted_iota(jnp.int32, (toks, width), 1)
    gap = row + halo - column
    allowed = (
        (query_seg == key_seg) & (gap >= 0) & (gap < window_ref[0]) & (column >= halo - c * toks)
    )
    mask[...] = jnp.where(allowed, 0.0, -jnp.inf)

    def far(rows, part):
        return sum(
            product(
                rows, slice(q * half + part * quarter, q * half + (part + 1) * quarter),
                wbuf[3, q, part * quarter : (part + 1) * quarter],
            )
            for q in range(2)
        )

    def relayed(part):
        pltpu.make_async_remote_copy(
            src_ref=wbuf.at[3, 0], dst_ref=wbuf.at[3, 0],
            send_sem=wsend, recv_sem=relay_recv.at[part],
            device_id=(mate, t), device_id_type=MESH,
        ).wait_recv()

    relayed(0)
    begun[0] = far(every, 0)
    relayed(1)
    for r in range(2):
        hand_over(3, r, begun[0, token_halves[r]] + far(token_halves[r], 1))

    def rows_of(step, r):
        return pl.ds((back - step) * span + r * toks, toks)

    def kv_copy(kind, src_step, dst_step, r, send, recv, to):
        return pltpu.make_async_remote_copy(
            src_ref=kv_ref.at[kind, rows_of(src_step, r)],
            dst_ref=kv_ref.at[kind, rows_of(dst_step, r)],
            send_sem=send, recv_sem=recv,
            device_id=(to, t), device_id_type=MESH,
        )

    def onward(step, r):
        to = jnp.minimum(2 * (pair + step) + core, n_ctx - 2 + core)
        return kv_copy(core, 0, step, r, ksend.at[step - 1], krecv.at[step - 1, r], to)

    def across(step, r):
        return kv_copy(core, step, step, r, fsend.at[step], frecv.at[step], mate)

    def crossed(step):
        block = kv_ref.at[1 - core, pl.ds((back - step) * span, span)]
        return pltpu.make_async_remote_copy(
            src_ref=block, dst_ref=block, send_sem=fsend.at[step], recv_sem=frecv.at[step],
            device_id=(mate, t), device_id_type=MESH,
        )

    def finish(rotated):
        bias = bias_ref[...].reshape(1, 2 * head).astype(jnp.float32)
        bias = bias[:, :head] if rotated else bias[:, head:]
        for r in range(2):
            rows = token_halves[r]
            total = own[rows] + bias
            for step in range(1, n_tp):
                source = (t + step) % n_tp
                pltpu.make_async_remote_copy(
                    src_ref=part_out.at[0, rows], dst_ref=part_in.at[source, rows],
                    send_sem=psend, recv_sem=precv.at[step - 1, r],
                    device_id=(c, source), device_id_type=MESH,
                ).wait_recv()
                total = total + part_in[source, rows].astype(jnp.float32)
            if rotated:
                total = total * cosb[rows] + pltpu.roll(total, head // 2, 1) * sinb[rows]
            kv_ref[0 if rotated else 1, rows_of(0, r), :] = total.astype(jnp.bfloat16)
            across(0, r).start()
            if rotated and r == 0:
                pl.semaphore_wait(clear, 1)
            for step in range(1, back + 1):
                @pl.when(pair + step < pairs)
                def _():
                    onward(step, r).start()

    def pass_on():
        for r in range(2):
            for step in range(1, back + 1):
                @pl.when(pair >= step)
                def _():
                    onward(step, r).wait_recv()
                    across(step, r).start()

    def await_crossed(steps):
        for step in steps:
            @pl.when(pair >= step)
            def _():
                crossed(step).wait_recv()

    def weigh(part, first, last, lower, upper):
        keys = kv_ref[0, pl.ds(pl.multiple_of(start + first, toks), last - first), :]
        scale = head ** (-0.5) * LOG2E

        def one(h):
            lanes = pl.ds(pl.multiple_of(h * head, head), head)
            scores = lax.dot_general(
                q_ref[:, lanes], keys, (((1,), (1,)), ((), ())), preferred_element_type=jnp.float32
            )
            scores = scores + mask[:, first:last]
            top = jnp.maximum(jnp.max(scores, axis=1, keepdims=True), LOWEST)
            weights = jnp.exp2((scores - top) * scale)
            tops[part, h] = top
            probs[h, :, first:last] = weights.astype(jnp.bfloat16)

        def couple(i, carry):
            one(2 * i)
            one(2 * i + 1)
            return carry

        lax.fori_loop(lower // 2, upper // 2, couple, 0)

    def mix_own(first):
        cache_ref[:, :head] = kv_ref[0, here, :]
        cache_ref[:, head:] = kv_ref[1, here, :]
        rows = pl.ds(pl.multiple_of(start + first, toks), width - first)
        values = jnp.concatenate(
            [kv_ref[1, rows, :], jnp.ones((width - first, head), jnp.bfloat16)], axis=1
        )

        def couple(i, carry):
            for h in (2 * i, 2 * i + 1):
                base[h] = jnp.dot(probs[h, :, first:], values, preferred_element_type=jnp.float32)
            return carry

        lax.fori_loop(0, group // 2, couple, 0)

    group = q_ref.shape[1] // head
    early = group // 4 * 2
    most = group * 3 // 8 * 2
    behind = pair - (n_tp - 1 - t)
    waits_long = (behind >= 1) & (behind <= back)

    @pl.when(core == 0)
    def _():
        finish(True)
        weigh(0, halo, width, 0, group)
        pass_on()
        weigh(1, 0, halo, 0, group)
        await_crossed([0])
        mix_own(halo)
        await_crossed(range(1, back + 1))

    @pl.when(core == 1)
    def _():
        split = halo - toks
        await_crossed([0])
        weigh(0, split, width, 0, group)
        is_last = (neighbour(n_tp - 1) == t) & (pair != back)

        @pl.when(is_last)
        def _():
            await_crossed(range(1, back + 1))
            weigh(1, 0, split, 0, early)
            finish(False)
            weigh(1, 0, split, early, group)
            pass_on()
            mix_own(split)

        @pl.when(jnp.logical_not(is_last))
        def _():
            finish(False)
            mix_own(split)
            await_crossed(range(1, back + 1))
            weigh(1, 0, split, 0, most)

            @pl.when(jnp.logical_not(waits_long))
            def _():
                pass_on()

            weigh(1, 0, split, most, group)

            @pl.when(waits_long)
            def _():
                pass_on()

    near[...] = kv_ref[1, pl.ds(start, halo), :]

    pltpu.make_async_remote_copy(
        src_ref=part_out.at[pl.ds(0, n_tp - 1)], dst_ref=part_in.at[pl.ds(0, n_tp - 1)],
        send_sem=psend, recv_sem=precv.at[0, 0], device_id=(mate, t), device_id_type=MESH,
    ).wait_send()

    def sent(sem):
        block = kv_ref.at[0, pl.ds(0, span)]
        pltpu.make_async_remote_copy(
            src_ref=block, dst_ref=block, send_sem=sem, recv_sem=krecv.at[0, 0],
            device_id=(mate, t), device_id_type=MESH,
        ).wait_send()

    sent(fsend.at[0])
    seg_block(0, 1).wait_send()
    for step in range(1, back + 1):
        @pl.when(pair + step < pairs)
        def _():
            sent(ksend.at[step - 1])
            seg_block(step, 2).wait_send()

        @pl.when(pair >= step)
        def _():
            sent(fsend.at[step])


def mix_kernel(probs, tops, base, near, cache_ref, out_hbm, cache_hbm, mixed, sems):
    group, toks, head = mixed.shape
    width = near.shape[0] + toks
    scale = head ** (-0.5) * LOG2E
    cache_copy = pltpu.make_async_copy(cache_ref, cache_hbm, sems.at[group])
    cache_copy.start()

    def out_copy(h):
        lanes = pl.ds(h * head, head)
        return pltpu.make_async_copy(mixed.at[h], out_hbm.at[:, lanes], sems.at[h])

    def mix(split):
        values = jnp.concatenate([near[:split], jnp.ones((split, head), near.dtype)], axis=1)
        for h in range(group):
            far = jnp.dot(probs[h, :, :split], values, preferred_element_type=jnp.float32)
            highest = jnp.maximum(tops[0, h], tops[1, h])
            lift = [jnp.exp2((tops[part, h] - highest) * scale) for part in range(2)]
            joint = base[h] * lift[0] + far * lift[1]
            mixed[h] = (joint[:, :head] / joint[:, head:]).astype(mixed.dtype)
            out_copy(h).start()

    core = lax.axis_index("ctx") % 2

    @pl.when(core == 0)
    def _():
        mix(width - toks)

    @pl.when(core == 1)
    def _():
        mix(width - 2 * toks)

    for h in range(group):
        out_copy(h).wait()
    cache_copy.wait()


def fast_body(halo, back, hidden, queries, kv_weight, kv_bias, window, segment_ids):
    toks, feats = hidden.shape
    head = kv_bias.shape[0] // 2
    span = 2 * toks
    group = queries.shape[1] // head
    n_tp = lax.axis_size("tp")
    freqs = rope_base ** (-2.0 * np.arange(head // 2, dtype=np.float64) / head)
    freqs = np.tile(np.concatenate([freqs, freqs])[None, :], (8, 1)).astype(np.float32)
    keys = (back + 1) * span
    vmem = pl.BlockSpec(memory_space=pltpu.VMEM)
    hbm = pl.BlockSpec(memory_space=pltpu.HBM)
    dma = pltpu.SemaphoreType.DMA
    width = halo + toks
    operands = [
        pltpu.with_memory_space_constraint(array, pltpu.HBM)
        for array in (hidden, kv_weight, queries, kv_bias, jnp.asarray(freqs), segment_ids)
    ]
    made = pl.pallas_call(
        functools.partial(fused_kernel, halo, back),
        out_shape=(
            pltpu.VMEM((group, toks, width), jnp.bfloat16),
            pltpu.VMEM((2, group, toks, 1), jnp.float32),
            pltpu.VMEM((group, toks, 2 * head), jnp.float32),
            pltpu.VMEM((halo, head), jnp.bfloat16),
            pltpu.VMEM((toks, 2 * head), jnp.bfloat16),
        ),
        in_specs=[pl.BlockSpec(memory_space=pltpu.SMEM), hbm, hbm, hbm, hbm, hbm, hbm],
        out_specs=(vmem,) * 5,
        scratch_shapes=[
            pltpu.VMEM((2, keys, head), jnp.bfloat16),
            pltpu.VMEM((8, keys), jnp.int32),
            pltpu.VMEM((span, feats), jnp.bfloat16),
            pltpu.VMEM((n_tp, 2, feats // 2, head), jnp.bfloat16),
            pltpu.VMEM((n_tp, span, head), jnp.bfloat16),
            pltpu.VMEM((n_tp, span, head), jnp.bfloat16),
            pltpu.VMEM((span, head), jnp.float32),
            pltpu.VMEM((span, head), jnp.float32),
            pltpu.VMEM((span, head), jnp.float32),
            pltpu.VMEM(queries.shape, jnp.bfloat16),
            pltpu.VMEM((2 * head,), jnp.bfloat16),
            pltpu.VMEM((8, head), jnp.float32),
            pltpu.VMEM((toks,), jnp.int32),
            pltpu.VMEM((8, toks), jnp.int32),
            pltpu.VMEM((toks, width), jnp.float32),
            pltpu.VMEM((2, span, head), jnp.float32),
            dma((7,)),
            dma((2,)),
            pltpu.SemaphoreType.REGULAR,
            pltpu.SemaphoreType.REGULAR,
            dma,
            dma((2, 2)),
            dma((2,)),
            dma,
            dma((n_tp - 1, 2)),
            dma((back,)),
            dma((back, 2)),
            dma((back + 1,)),
            dma((back + 1,)),
            dma((back + 1,)),
            dma((back + 1,)),
        ],
        compiler_params=pltpu.CompilerParams(
            collective_id=0, has_side_effects=True, vmem_limit_bytes=32 << 20
        ),
    )(window, *operands)
    made = [pltpu.with_memory_space_constraint(array, pltpu.VMEM) for array in made]
    return pl.pallas_call(
        mix_kernel,
        out_shape=(
            jax.ShapeDtypeStruct(queries.shape, jnp.bfloat16),
            jax.ShapeDtypeStruct((toks, 2 * head), jnp.bfloat16),
        ),
        in_specs=[vmem] * 5,
        out_specs=(hbm, hbm),
        scratch_shapes=[pltpu.VMEM((group, toks, head), jnp.bfloat16), dma((group + 1,))],
        compiler_params=pltpu.CompilerParams(vmem_limit_bytes=32 << 20),
    )(*made)


def solution(mesh):
    in_specs = (P("ctx", "tp"), P("ctx", "tp"), P("tp", "ctx"), P("tp"), P("tp"), P("ctx"))
    out_specs = (P("ctx", "tp"), P("ctx", "tp"))
    n_ctx, n_tp = mesh.shape["ctx"], mesh.shape["tp"]

    def step(hidden, queries, kv_weight, kv_bias, window, segment_ids):
        toks = hidden.shape[0]
        args = (hidden, queries, kv_weight, kv_bias, window, segment_ids)
        if n_ctx != 8 or n_ctx != 2 * n_tp or 2 * kv_weight.shape[1] != kv_bias.shape[0]:
            return body(*args)
        longest = min(WINDOW, n_ctx * toks // 2)
        blocks = -(-(longest - 1) // toks)
        return fast_body(blocks * toks, -(-blocks // 2), *args)

    return jax.shard_map(step, mesh=mesh, in_specs=in_specs, out_specs=out_specs, check_vma=False)
```

```python
import functools

import jax
import jax.numpy as jnp
import numpy as np
from jax import lax
from jax.experimental import pallas as pl
from jax.experimental.pallas import tpu as pltpu
from jax.sharding import PartitionSpec as P

WINDOW = 4096
MESH = pl.DeviceIdType.MESH
LOG2E = 1.4426950408889634
LOWEST = -1e30


rope_base = 1000000.0


def passed_along(value, axis, steps):
    count = lax.axis_size(axis)
    initial, last = (max(0, -steps), min(count, count - steps))
    return lax.ppermute(value, axis, [(source, source + steps) for source in range(initial, last)])


def rotate(values, positions):
    half = values.shape[-1] // 2
    freqs = rope_base ** (-2.0 * jnp.arange(half, dtype=jnp.float32) / values.shape[-1])
    angles = positions.astype(jnp.float32)[:, None] * freqs[None, :]
    cosine = jnp.cos(angles)
    sine = jnp.sin(angles)
    former = values[:, :half]
    latter = values[:, half:]
    return jnp.concatenate(
        [former * cosine - latter * sine, latter * cosine + former * sine], axis=1
    )


def attend(carry, query_rows, query_pos, query_seg, reach, block, block_seg, block_pos):
    running_max, running_sum, weighted = carry
    head = block.shape[1] // 2
    scores = lax.dot_general(
        query_rows, block[:, :head], (((1,), (1,)), ((), ())), preferred_element_type=jnp.float32
    )
    scores = scores * head ** (-0.5)
    gap = query_pos[:, None] - block_pos[None, :]
    allowed = (
        (query_seg[:, None] == block_seg[None, :])
        & (gap >= 0)
        & (gap < reach)
        & (block_pos >= 0)[None, :]
    )
    scores = jnp.where(allowed, scores, -jnp.inf)
    newest = jnp.maximum(running_max, jnp.max(scores, axis=1))
    probs = jnp.exp(scores - newest[:, None])
    rescale = jnp.exp(running_max - newest)
    summed = running_sum * rescale + jnp.sum(probs, axis=1)
    mixed = jnp.dot(probs.astype(jnp.bfloat16), block[:, head:], preferred_element_type=jnp.float32)
    return (newest, summed, weighted * rescale[:, None] + mixed)


def body(hidden, queries, kv_weight, kv_bias, window, segment_ids):
    tok_rows = hidden.shape[0]
    terms = jnp.dot(
        hidden,
        lax.all_gather(kv_weight, "ctx", axis=1, tiled=True),
        preferred_element_type=jnp.float32,
    )
    projected = lax.psum_scatter(terms, "tp", scatter_dimension=1, tiled=True)
    projected = projected + kv_bias.astype(jnp.float32)[None, :]
    head = kv_bias.shape[0] // 2
    shard = lax.axis_index("ctx")
    offsets = jnp.arange(tok_rows, dtype=jnp.int32)
    positions = shard * tok_rows + offsets
    cache = jnp.concatenate(
        [rotate(projected[:, :head], positions), projected[:, head:]], axis=1
    ).astype(jnp.bfloat16)
    group = queries.shape[1] // head
    query_rows = queries.reshape(tok_rows * group, head)
    query_pos = jnp.repeat(positions, group)
    query_seg = jnp.repeat(segment_ids, group)
    reach = window[0]

    def absorb(carry, block, block_seg, block_pos):
        return attend(carry, query_rows, query_pos, query_seg, reach, block, block_seg, block_pos)

    row_count = tok_rows * group
    carry = (
        jnp.full((row_count,), -jnp.inf, jnp.float32),
        jnp.zeros((row_count,), jnp.float32),
        jnp.zeros((row_count, head), jnp.float32),
    )
    carry = absorb(carry, cache, segment_ids, positions)
    halo_count = WINDOW // tok_rows
    held_kv = cache
    held_seg = segment_ids
    have = 0
    while have < halo_count:
        got_kv, got_seg = passed_along((held_kv, held_seg), "ctx", max(have, 1))
        shards = got_kv.shape[0] // tok_rows
        for member in range(shards):
            lower = member * tok_rows
            block_pos = (shard - have - shards + member) * tok_rows + offsets
            carry = absorb(
                carry,
                got_kv[lower : lower + tok_rows],
                got_seg[lower : lower + tok_rows],
                block_pos,
            )
        if have == 0:
            held_kv, held_seg = (got_kv, got_seg)
        else:
            held_kv = jnp.concatenate([got_kv, held_kv], axis=0)
            held_seg = jnp.concatenate([got_seg, held_seg], axis=0)
        have = have + shards
    newest, summed, weighted = carry
    attended = (weighted / summed[:, None]).reshape(tok_rows, group * head).astype(jnp.bfloat16)
    return (attended, cache)


def fused_kernel(
    halo, back, window_ref, hid_hbm, w_hbm, q_hbm, bias_hbm, freq_hbm, seg_hbm,
    probs, tops, base, near, cache_ref,
    kv_ref, segs_ref, hbuf, wbuf, part_out, part_in, own, cosb, sinb,
    q_ref, bias_ref, freq_ref, seg_line, seg_ref, mask, begun,
    local_sem, hid_sem, gate, clear, wsend, wrecv, relay_recv, psend, precv, ksend, krecv, fsend, frecv, ssend, srecv,
):
    c = lax.axis_index("ctx")
    t = lax.axis_index("tp")
    n_ctx = lax.axis_size("ctx")
    n_tp = lax.axis_size("tp")
    pairs = n_ctx // 2
    pair = c // 2
    core = c % 2
    mate = pair * 2 + (1 - core)
    toks = hid_hbm.shape[0]
    feats, head = w_hbm.shape
    half = feats // 2
    span = 2 * toks
    own_rows = pl.ds(pl.multiple_of(core * toks, toks), toks)

    load_w = [
        pltpu.make_async_copy(w_hbm.at[pl.ds(q * half, half)], wbuf.at[0, q], local_sem.at[q])
        for q in range(2)
    ]
    load_h = pltpu.make_async_copy(hid_hbm, hbuf.at[own_rows], local_sem.at[2])
    small = [
        pltpu.make_async_copy(src, dst, local_sem.at[3 + at])
        for at, (src, dst) in enumerate(
            [(seg_hbm, seg_line), (bias_hbm, bias_ref), (freq_hbm, freq_ref), (q_hbm, q_ref)]
        )
    ]
    load_w[0].start()
    load_w[1].start()
    load_h.start()
    for copy in small:
        copy.start()

    barrier = pltpu.get_barrier_semaphore()
    for step in range(1, n_ctx):
        pl.semaphore_signal(barrier, inc=1, device_id=((c + step) % n_ctx, t), device_id_type=MESH)
    for step in range(1, n_tp):
        pl.semaphore_signal(barrier, inc=1, device_id=(c, (t + step) % n_tp), device_id_type=MESH)
    pl.semaphore_wait(barrier, n_ctx + n_tp - 2)

    def neighbour(d):
        other_x = 1 - pair % 2 if d % 2 else pair % 2
        other_y = 1 - pair // 2 if d // 2 else pair // 2
        return other_y * 2 + other_x

    def w_copy(src, dst, q, to):
        return pltpu.make_async_remote_copy(
            src_ref=wbuf.at[src, q], dst_ref=wbuf.at[dst, q],
            send_sem=wsend, recv_sem=wrecv.at[dst - 1, q],
            device_id=(2 * neighbour(to) + core, t), device_id_type=MESH,
        )

    x_first, x_second = w_copy(0, 1, 0, 1), w_copy(0, 1, 1, 1)
    y_first, y_second = w_copy(0, 2, 1, 2), w_copy(0, 2, 0, 2)
    quarter = half // 2

    def relay_copy(src, q, part, to):
        rows = pl.ds(part * quarter, quarter)
        return pltpu.make_async_remote_copy(
            src_ref=wbuf.at[src, q, rows], dst_ref=wbuf.at[3, q, rows],
            send_sem=wsend, recv_sem=relay_recv.at[part],
            device_id=(2 * neighbour(to) + core, t), device_id_type=MESH,
        )

    relay_y = [relay_copy(1, 0, part, 2) for part in range(2)]
    relay_x = [relay_copy(2, 1, part, 1) for part in range(2)]

    def send_weights():
        x_first.start()
        y_first.start()
        x_second.start()
        y_second.start()

    load_w[0].wait()
    load_w[1].wait()

    @pl.when(core == 0)
    def _():
        send_weights()

    load_h.wait()
    hid = pltpu.make_async_remote_copy(
        src_ref=hbuf.at[own_rows], dst_ref=hbuf.at[own_rows],
        send_sem=hid_sem.at[0], recv_sem=hid_sem.at[1], device_id=(mate, t), device_id_type=MESH,
    )
    hid.start()
    for copy in small:
        copy.wait()
    seg_ref[...] = jnp.broadcast_to(seg_line[...].reshape(1, toks), seg_ref.shape)

    def seg_copy(step, sub):
        at = pl.ds(pl.multiple_of((back - step) * span + core * toks, toks), toks)
        return pltpu.make_async_remote_copy(
            src_ref=seg_ref, dst_ref=segs_ref.at[:, at],
            send_sem=ssend.at[step], recv_sem=srecv.at[step],
            device_id=(jnp.minimum(2 * (pair + step) + sub, n_ctx - 1) if step else mate, t),
            device_id_type=MESH,
        )

    for step in range(back + 1):
        if step == 0:
            segs_ref[:, pl.ds(pl.multiple_of(back * span + core * toks, toks), toks)] = seg_ref[...]
            seg_copy(0, 0).start()
        else:
            @pl.when(pair + step < pairs)
            def _():
                seg_copy(step, 0).start()
                seg_copy(step, 1).start()

            @pl.when(pair < step)
            def _():
                rows = slice((back - step) * span, (back - step + 1) * span)
                segs_ref[:, rows] = jnp.full((segs_ref.shape[0], span), -1, jnp.int32)
                kv_ref[:, rows, :] = jnp.zeros((2, span, head), jnp.bfloat16)

    low, high = slice(0, toks), slice(toks, span)
    token_halves = (low, high)

    def product(rows, features, weights):
        return jnp.dot(hbuf[rows, features], weights, preferred_element_type=jnp.float32)

    def part_copy(d, r):
        return pltpu.make_async_remote_copy(
            src_ref=part_out.at[d, token_halves[r]], dst_ref=part_in.at[t, token_halves[r]],
            send_sem=psend, recv_sem=precv.at[(t - neighbour(d) + n_tp - 1) % n_tp, r],
            device_id=(c, neighbour(d)), device_id_type=MESH,
        )

    def hand_over(d, r, acc):
        rows = token_halves[r]
        part_out[d, rows] = acc.astype(part_out.dtype)

        @pl.when(neighbour(d) == t)
        def _():
            own[rows] = acc

        @pl.when(neighbour(d) != t)
        def _():
            part_copy(d, r).start()

    def whole(q):
        return slice(q * half, (q + 1) * half)

    hid.wait()
    every = slice(0, span)
    local = product(every, whole(0), wbuf[0, 0]) + product(every, whole(1), wbuf[0, 1])
    for r in range(2):
        hand_over(0, r, local[token_halves[r]])

    @pl.when(core == 1)
    def _():
        pl.semaphore_wait(gate, 1)
        send_weights()

    x_first.wait_recv()
    for copy in relay_y:
        copy.start()
    y_first.wait_recv()
    for copy in relay_x:
        copy.start()

    angle_rows = (lax.broadcasted_iota(jnp.int32, (span, head), 0) + pair * span).astype(jnp.float32)
    angles = angle_rows * freq_ref[0:1, :]
    is_key = core == 0
    left = lax.broadcasted_iota(jnp.int32, (span, head), 1) < head // 2
    sine = jnp.sin(angles)
    cosb[...] = jnp.where(is_key, jnp.cos(angles), 1.0)
    sinb[...] = jnp.where(is_key, jnp.where(left, -sine, sine), 0.0)

    for d in (1, 2):
        begun[d - 1] = product(every, whole(d - 1), wbuf[d, d - 1])
    y_second.wait_recv()
    x_second.wait_recv()

    @pl.when(core == 0)
    def _():
        pl.semaphore_signal(gate, inc=1, device_id=(mate, t), device_id_type=MESH)

    for d in (2, 1):
        full = begun[d - 1] + product(every, whole(2 - d), wbuf[d, 2 - d])
        for r in range(2):
            hand_over(d, r, full[token_halves[r]])
    pltpu.make_async_remote_copy(
        src_ref=wbuf.at[pl.ds(0, 3)], dst_ref=wbuf.at[pl.ds(0, 3)],
        send_sem=wsend, recv_sem=wrecv.at[0, 0], device_id=(mate, t), device_id_type=MESH,
    ).wait_send()

    @pl.when(core == 1)
    def _():
        pl.semaphore_signal(clear, inc=1, device_id=(mate, t), device_id_type=MESH)

    def seg_block(step, count):
        block = segs_ref.at[:, pl.ds((back - step) * span, count * toks)]
        return pltpu.make_async_remote_copy(
            src_ref=block, dst_ref=block, send_sem=ssend.at[step], recv_sem=srecv.at[step],
            device_id=(mate, t), device_id_type=MESH,
        )

    seg_block(0, 1).wait_recv()
    for step in range(1, back + 1):
        @pl.when(pair >= step)
        def _():
            seg_block(step, 2).wait_recv()

    width = halo + toks
    start = pl.multiple_of((core + 2 * back) * toks - halo, toks)
    here = pl.ds(pl.multiple_of((core + 2 * back) * toks, toks), toks)
    key_seg = segs_ref[0:1, pl.ds(start, width)]
    query_seg = jnp.transpose(jnp.broadcast_to(seg_ref[0:1, :], (head, toks)))[:, 0:1]
    row = lax.broadcasted_iota(jnp.int32, (toks, width), 0)
    column = lax.broadcasted_iota(jnp.int32, (toks, width), 1)
    gap = row + halo - column
    allowed = (
        (query_seg == key_seg) & (gap >= 0) & (gap < window_ref[0]) & (column >= halo - c * toks)
    )
    mask[...] = jnp.where(allowed, 0.0, -jnp.inf)

    def far(rows, part):
        return sum(
            product(
                rows, slice(q * half + part * quarter, q * half + (part + 1) * quarter),
                wbuf[3, q, part * quarter : (part + 1) * quarter],
            )
            for q in range(2)
        )

    def relayed(part):
        pltpu.make_async_remote_copy(
            src_ref=wbuf.at[3, 0], dst_ref=wbuf.at[3, 0],
            send_sem=wsend, recv_sem=relay_recv.at[part],
            device_id=(mate, t), device_id_type=MESH,
        ).wait_recv()

    relayed(0)
    begun[0] = far(every, 0)
    relayed(1)
    for r in range(2):
        hand_over(3, r, begun[0, token_halves[r]] + far(token_halves[r], 1))

    def rows_of(step, r):
        return pl.ds((back - step) * span + r * toks, toks)

    def kv_copy(kind, src_step, dst_step, r, send, recv, to):
        return pltpu.make_async_remote_copy(
            src_ref=kv_ref.at[kind, rows_of(src_step, r)],
            dst_ref=kv_ref.at[kind, rows_of(dst_step, r)],
            send_sem=send, recv_sem=recv,
            device_id=(to, t), device_id_type=MESH,
        )

    def onward(step, r):
        to = jnp.minimum(2 * (pair + step) + core, n_ctx - 2 + core)
        return kv_copy(core, 0, step, r, ksend.at[step - 1], krecv.at[step - 1, r], to)

    def across(step, r):
        return kv_copy(core, step, step, r, fsend.at[step], frecv.at[step], mate)

    def crossed(step):
        block = kv_ref.at[1 - core, pl.ds((back - step) * span, span)]
        return pltpu.make_async_remote_copy(
            src_ref=block, dst_ref=block, send_sem=fsend.at[step], recv_sem=frecv.at[step],
            device_id=(mate, t), device_id_type=MESH,
        )

    def finish(rotated):
        bias = bias_ref[...].reshape(1, 2 * head).astype(jnp.float32)
        bias = bias[:, :head] if rotated else bias[:, head:]
        for r in range(2):
            rows = token_halves[r]
            total = own[rows] + bias
            for step in range(1, n_tp):
                source = (t + step) % n_tp
                pltpu.make_async_remote_copy(
                    src_ref=part_out.at[0, rows], dst_ref=part_in.at[source, rows],
                    send_sem=psend, recv_sem=precv.at[step - 1, r],
                    device_id=(c, source), device_id_type=MESH,
                ).wait_recv()
                total = total + part_in[source, rows].astype(jnp.float32)
            if rotated:
                total = total * cosb[rows] + pltpu.roll(total, head // 2, 1) * sinb[rows]
            kv_ref[0 if rotated else 1, rows_of(0, r), :] = total.astype(jnp.bfloat16)
            across(0, r).start()
            if rotated and r == 0:
                pl.semaphore_wait(clear, 1)
            for step in range(1, back + 1):
                @pl.when(pair + step < pairs)
                def _():
                    onward(step, r).start()

    def pass_on():
        for r in range(2):
            for step in range(1, back + 1):
                @pl.when(pair >= step)
                def _():
                    onward(step, r).wait_recv()
                    across(step, r).start()

    def await_crossed(steps):
        for step in steps:
            @pl.when(pair >= step)
            def _():
                crossed(step).wait_recv()

    def weigh(part, first, last, lower, upper):
        keys = kv_ref[0, pl.ds(pl.multiple_of(start + first, toks), last - first), :]
        scale = head ** (-0.5) * LOG2E

        def one(h):
            lanes = pl.ds(pl.multiple_of(h * head, head), head)
            scores = lax.dot_general(
                q_ref[:, lanes], keys, (((1,), (1,)), ((), ())), preferred_element_type=jnp.float32
            )
            scores = scores + mask[:, first:last]
            top = jnp.maximum(jnp.max(scores, axis=1, keepdims=True), LOWEST)
            weights = jnp.exp2((scores - top) * scale)
            tops[part, h] = top
            probs[h, :, first:last] = weights.astype(jnp.bfloat16)

        some = 4 if (upper - lower) % 4 == 0 else 2

        def several(i, carry):
            for at in range(some):
                one(lower + some * i + at)
            return carry

        lax.fori_loop(0, (upper - lower) // some, several, 0)

    def mix_own(first):
        cache_ref[:, :head] = kv_ref[0, here, :]
        cache_ref[:, head:] = kv_ref[1, here, :]
        rows = pl.ds(pl.multiple_of(start + first, toks), width - first)
        values = jnp.concatenate(
            [kv_ref[1, rows, :], jnp.ones((width - first, head), jnp.bfloat16)], axis=1
        )

        for h in range(group):
            base[h] = jnp.dot(probs[h, :, first:], values, preferred_element_type=jnp.float32)

    group = q_ref.shape[1] // head
    early = group // 4 * 2
    most = group * 3 // 8 * 2
    behind = pair - (n_tp - 1 - t)
    waits_long = (behind >= 1) & (behind <= back)

    @pl.when(core == 0)
    def _():
        finish(True)
        weigh(0, halo, width, 0, group)
        pass_on()
        weigh(1, 0, halo, 0, group)
        await_crossed([0])
        mix_own(halo)
        await_crossed(range(1, back + 1))

    @pl.when(core == 1)
    def _():
        split = halo - toks
        await_crossed([0])
        weigh(0, split, width, 0, group)
        is_last = neighbour(n_tp - 1) == t
        is_early = is_last & (pair != back)
        is_end = pair == pairs - 1

        def late_order(ahead):
            await_crossed(range(1, back + 1))
            weigh(1, 0, split, 0, ahead)
            finish(False)
            weigh(1, 0, split, ahead, group)
            pass_on()
            mix_own(split)

        @pl.when(is_early & jnp.logical_not(is_end))
        def _():
            late_order(early)

        @pl.when(is_early & is_end)
        def _():
            late_order(most)

        @pl.when(jnp.logical_not(is_early))
        def _():
            finish(False)

            @pl.when(jnp.logical_not(is_last))
            def _():
                mix_own(split)

            await_crossed(range(1, back + 1))
            weigh(1, 0, split, 0, most)

            @pl.when(jnp.logical_not(waits_long))
            def _():
                pass_on()

            weigh(1, 0, split, most, group)

            @pl.when(waits_long)
            def _():
                pass_on()

            @pl.when(is_last)
            def _():
                mix_own(split)

    near[...] = kv_ref[1, pl.ds(start, halo), :]

    pltpu.make_async_remote_copy(
        src_ref=part_out.at[pl.ds(0, n_tp - 1)], dst_ref=part_in.at[pl.ds(0, n_tp - 1)],
        send_sem=psend, recv_sem=precv.at[0, 0], device_id=(mate, t), device_id_type=MESH,
    ).wait_send()

    def sent(sem):
        block = kv_ref.at[0, pl.ds(0, span)]
        pltpu.make_async_remote_copy(
            src_ref=block, dst_ref=block, send_sem=sem, recv_sem=krecv.at[0, 0],
            device_id=(mate, t), device_id_type=MESH,
        ).wait_send()

    sent(fsend.at[0])
    seg_block(0, 1).wait_send()
    for step in range(1, back + 1):
        @pl.when(pair + step < pairs)
        def _():
            sent(ksend.at[step - 1])
            seg_block(step, 2).wait_send()

        @pl.when(pair >= step)
        def _():
            sent(fsend.at[step])


def mix_kernel(probs, tops, base, near, cache_ref, out_hbm, cache_hbm, mixed, sems):
    group, toks, head = mixed.shape
    width = near.shape[0] + toks
    scale = head ** (-0.5) * LOG2E
    cache_copy = pltpu.make_async_copy(cache_ref, cache_hbm, sems.at[group])
    cache_copy.start()

    def out_copy(h):
        lanes = pl.ds(h * head, head)
        return pltpu.make_async_copy(mixed.at[h], out_hbm.at[:, lanes], sems.at[h])

    def mix(split):
        values = jnp.concatenate([near[:split], jnp.ones((split, head), near.dtype)], axis=1)
        for h in range(group):
            far = jnp.dot(probs[h, :, :split], values, preferred_element_type=jnp.float32)
            highest = jnp.maximum(tops[0, h], tops[1, h])
            lift = [jnp.exp2((tops[part, h] - highest) * scale) for part in range(2)]
            joint = base[h] * lift[0] + far * lift[1]
            mixed[h] = (joint[:, :head] / joint[:, head:]).astype(mixed.dtype)
            out_copy(h).start()

    core = lax.axis_index("ctx") % 2

    @pl.when(core == 0)
    def _():
        mix(width - toks)

    @pl.when(core == 1)
    def _():
        mix(width - 2 * toks)

    for h in range(group):
        out_copy(h).wait()
    cache_copy.wait()


def fast_body(halo, back, hidden, queries, kv_weight, kv_bias, window, segment_ids):
    toks, feats = hidden.shape
    head = kv_bias.shape[0] // 2
    span = 2 * toks
    group = queries.shape[1] // head
    n_tp = lax.axis_size("tp")
    freqs = rope_base ** (-2.0 * np.arange(head // 2, dtype=np.float64) / head)
    freqs = np.tile(np.concatenate([freqs, freqs])[None, :], (8, 1)).astype(np.float32)
    keys = (back + 1) * span
    vmem = pl.BlockSpec(memory_space=pltpu.VMEM)
    hbm = pl.BlockSpec(memory_space=pltpu.HBM)
    dma = pltpu.SemaphoreType.DMA
    width = halo + toks
    operands = [
        pltpu.with_memory_space_constraint(array, pltpu.HBM)
        for array in (hidden, kv_weight, queries, kv_bias, jnp.asarray(freqs), segment_ids)
    ]
    made = pl.pallas_call(
        functools.partial(fused_kernel, halo, back),
        out_shape=(
            pltpu.VMEM((group, toks, width), jnp.bfloat16),
            pltpu.VMEM((2, group, toks, 1), jnp.float32),
            pltpu.VMEM((group, toks, 2 * head), jnp.float32),
            pltpu.VMEM((halo, head), jnp.bfloat16),
            pltpu.VMEM((toks, 2 * head), jnp.bfloat16),
        ),
        in_specs=[pl.BlockSpec(memory_space=pltpu.SMEM), hbm, hbm, hbm, hbm, hbm, hbm],
        out_specs=(vmem,) * 5,
        scratch_shapes=[
            pltpu.VMEM((2, keys, head), jnp.bfloat16),
            pltpu.VMEM((8, keys), jnp.int32),
            pltpu.VMEM((span, feats), jnp.bfloat16),
            pltpu.VMEM((n_tp, 2, feats // 2, head), jnp.bfloat16),
            pltpu.VMEM((n_tp, span, head), jnp.bfloat16),
            pltpu.VMEM((n_tp, span, head), jnp.bfloat16),
            pltpu.VMEM((span, head), jnp.float32),
            pltpu.VMEM((span, head), jnp.float32),
            pltpu.VMEM((span, head), jnp.float32),
            pltpu.VMEM(queries.shape, jnp.bfloat16),
            pltpu.VMEM((2 * head,), jnp.bfloat16),
            pltpu.VMEM((8, head), jnp.float32),
            pltpu.VMEM((toks,), jnp.int32),
            pltpu.VMEM((8, toks), jnp.int32),
            pltpu.VMEM((toks, width), jnp.float32),
            pltpu.VMEM((2, span, head), jnp.float32),
            dma((7,)),
            dma((2,)),
            pltpu.SemaphoreType.REGULAR,
            pltpu.SemaphoreType.REGULAR,
            dma,
            dma((2, 2)),
            dma((2,)),
            dma,
            dma((n_tp - 1, 2)),
            dma((back,)),
            dma((back, 2)),
            dma((back + 1,)),
            dma((back + 1,)),
            dma((back + 1,)),
            dma((back + 1,)),
        ],
        compiler_params=pltpu.CompilerParams(
            collective_id=0, has_side_effects=True, vmem_limit_bytes=32 << 20
        ),
    )(window, *operands)
    made = [pltpu.with_memory_space_constraint(array, pltpu.VMEM) for array in made]
    return pl.pallas_call(
        mix_kernel,
        out_shape=(
            jax.ShapeDtypeStruct(queries.shape, jnp.bfloat16),
            jax.ShapeDtypeStruct((toks, 2 * head), jnp.bfloat16),
        ),
        in_specs=[vmem] * 5,
        out_specs=(hbm, hbm),
        scratch_shapes=[pltpu.VMEM((group, toks, head), jnp.bfloat16), dma((group + 1,))],
        compiler_params=pltpu.CompilerParams(vmem_limit_bytes=32 << 20),
    )(*made)


def solution(mesh):
    in_specs = (P("ctx", "tp"), P("ctx", "tp"), P("tp", "ctx"), P("tp"), P("tp"), P("ctx"))
    out_specs = (P("ctx", "tp"), P("ctx", "tp"))
    n_ctx, n_tp = mesh.shape["ctx"], mesh.shape["tp"]

    def step(hidden, queries, kv_weight, kv_bias, window, segment_ids):
        toks = hidden.shape[0]
        args = (hidden, queries, kv_weight, kv_bias, window, segment_ids)
        if n_ctx != 8 or n_ctx != 2 * n_tp or 2 * kv_weight.shape[1] != kv_bias.shape[0]:
            return body(*args)
        longest = min(WINDOW, n_ctx * toks // 2)
        blocks = -(-(longest - 1) // toks)
        return fast_body(blocks * toks, -(-blocks // 2), *args)

    return jax.shard_map(step, mesh=mesh, in_specs=in_specs, out_specs=out_specs, check_vma=False)
```
